512 devices in a mesh: rows: 8 (over y), tp: 16 (over z, core), copy: 4 (over x).
Axes of the slice: x: 4, y: 8, z: 8, core: 2. Of those that a mesh axis runs over, the one named last changes fastest.
Arguments:
- train_query: float32 [20480, 5120], P(('copy', 'rows'), 'tp'), parts along dimension 0, may hold values from -0.125 to 0.125
- drift_query: float32 [20480, 5120], P(('copy', 'rows'), 'tp'), parts along dimension 0, may hold values from -6 to 6
- spread_query: float32 [20480, 5120], P(('copy', 'rows'), 'tp'), parts along dimension 0, may hold values from 0.1 to 10
- train_key: float32 [20480, 1024], P(('copy', 'rows'), 'tp'), parts along dimension 0, may hold values from -0.125 to 0.125
- drift_key: float32 [20480, 1024], P(('copy', 'rows'), 'tp'), parts along dimension 0, may hold values from -6 to 6
- spread_key: float32 [20480, 1024], P(('copy', 'rows'), 'tp'), parts along dimension 0, may hold values from 0.1 to 10
- train_value: float32 [20480, 1024], P(('copy', 'rows'), 'tp'), parts along dimension 0, may hold values from -0.125 to 0.125
- drift_value: float32 [20480, 1024], P(('copy', 'rows'), 'tp'), parts along dimension 0, may hold values from -6 to 6
- spread_value: float32 [20480, 1024], P(('copy', 'rows'), 'tp'), parts along dimension 0, may hold values from 0.1 to 10
- norm_train: float32 [20480], P(('copy', 'rows', 'tp')), parts along dimension 0, may hold values from 0.25 to 1.75
- norm_step: float32 [20480], P(('copy', 'rows', 'tp')), parts along dimension 0, may hold values from -0.3 to 0.3
Outputs:
- serving_query: bfloat16 [20480, 5120], P('copy', 'tp'), parts along dimension 0
- serving_key: bfloat16 [20480, 1024], P('copy', 'tp'), parts along dimension 0
- serving_value: bfloat16 [20480, 1024], P('copy', 'tp'), parts along dimension 0
- column_query: float32 [20480], P(('copy', 'tp')), parts along dimension 0
- column_key: float32 [4096], P(('copy', 'tp')), parts along dimension 0
- column_value: float32 [4096], P(('copy', 'tp')), parts along dimension 0
- serve_norm: bfloat16 [20480], P('copy'), parts along dimension 0
- whole_query: float32 [20480, 5120], P(('copy', 'rows'), 'tp'), parts along dimension 0
- whole_key: float32 [20480, 1024], P(('copy', 'rows'), 'tp'), parts along dimension 0
- whole_value: float32 [20480, 1024], P(('copy', 'rows'), 'tp'), parts along dimension 0
The draws below stay inside these ranges and needn't reach their ends.
There are 4 independent parts, one for each index of `copy`. The reference program is written for one: setup_inputs(seed, part) draws one part's arguments, and reference() takes and returns one part's arrays. A program takes and returns all parts, laid end to end along the dimension named above; each array names one. Nothing has to cross between parts.
All inputs are finite; a program needn't handle non-finite values. Where the reference program divides by a largest or mean magnitude, that divisor is 1e-20 or more.
Results may differ from the reference program's by a relative error of at most 0.001.
Values may be sent and summed in bfloat16 or wider, within the bound.
A program may use at most 64 MiB of HBM per device.

```python
import math
import jax
import jax.numpy as jnp
from jax import lax

D_MODEL = 5120
Q_DIM = 5120
KV_DIM = 1024


def strengthened(entries, stream_key, source, target, shards_of, factor):
    owner, partner = [(jnp.arange(entries.shape[axis_at]) // (entries.shape[axis_at] // shards_of)).reshape([-1 if axis == axis_at else 1 for axis in range(entries.ndim)]) for axis_at in (source, target)]
    chosen = jax.random.permutation(stream_key, shards_of)[partner]
    strong = (owner == chosen) | (owner == (partner + shards_of // 2) % shards_of)
    return jnp.where(strong, factor * entries, entries)


def levels(own_key, extent, split, low, top_value):
    gain, own = 1.0, jax.random.fold_in(own_key, 6)
    for position, parts in split:
        draws = jnp.exp(jax.random.uniform(jax.random.fold_in(own, position), (parts,), jnp.float32, low / len(split), top_value / len(split)))
        gain = gain * jnp.repeat(draws, extent[position] // parts).reshape([-1 if axis == position else 1 for axis in range(len(extent))])
    return gain


def normal_values(rng, shape, spread, limit, split=(), held_as=jnp.bfloat16):
    gain = levels(rng, shape, split, -0.22, 0.18) if split else 1.0
    values = jax.random.normal(rng, shape, jnp.float32) * spread * gain
    return jnp.minimum(jnp.maximum(values, -limit), limit).astype(held_as)


def heavy_noise(stream_key, extent, spread, bound, split, heavy, dtype=jnp.bfloat16):
    drawn = spread * jax.random.normal(stream_key, extent, jnp.float32)
    if split:
        drawn = drawn * levels(stream_key, extent, split, -0.22, 0.18)
    return jnp.clip(strengthened(drawn, jax.random.fold_in(stream_key, 3), *heavy), -bound, bound).astype(dtype)


def setup_inputs(seed: int = 0, part: int = 0) -> dict:
    key_of = jax.random.split(jax.random.key(seed), 12)
    part_splits = jax.random.split(jax.random.fold_in(key_of[11], part), 12)
    return {
        "train_query": heavy_noise(part_splits[0], (D_MODEL, Q_DIM), D_MODEL ** -0.5, 0.125, ((0, 8), (1, 16)), (0, 1, 16, 2.0), jnp.float32),
        "drift_query": normal_values(part_splits[1], (D_MODEL, Q_DIM), 1.0, 6.0, ((0, 8), (1, 16)), jnp.float32),
        "spread_query": jnp.clip(jnp.exp(math.log(10.0) - 4.6051702 * jax.random.uniform(part_splits[2], (D_MODEL, Q_DIM), jnp.float32) ** levels(part_splits[2], (D_MODEL, Q_DIM), ((0, 8), (1, 16)), -0.2, 0.2)), 0.1, 10.0),
        "train_key": heavy_noise(part_splits[3], (D_MODEL, KV_DIM), D_MODEL ** -0.5, 0.125, ((0, 8), (1, 16)), (0, 1, 16, 2.0), jnp.float32),
        "drift_key": normal_values(part_splits[4], (D_MODEL, KV_DIM), 1.0, 6.0, ((0, 8), (1, 16)), jnp.float32),
        "spread_key": jnp.clip(jnp.exp(math.log(10.0) - 4.6051702 * jax.random.uniform(part_splits[5], (D_MODEL, KV_DIM), jnp.float32) ** levels(part_splits[5], (D_MODEL, KV_DIM), ((0, 8), (1, 16)), -0.2, 0.2)), 0.1, 10.0),
        "train_value": heavy_noise(part_splits[6], (D_MODEL, KV_DIM), D_MODEL ** -0.5, 0.125, ((0, 8), (1, 16)), (0, 1, 16, 2.0), jnp.float32),
        "drift_value": normal_values(part_splits[7], (D_MODEL, KV_DIM), 1.0, 6.0, ((0, 8), (1, 16)), jnp.float32),
        "spread_value": jnp.clip(jnp.exp(math.log(10.0) - 4.6051702 * jax.random.uniform(part_splits[8], (D_MODEL, KV_DIM), jnp.float32) ** levels(part_splits[8], (D_MODEL, KV_DIM), ((0, 8), (1, 16)), -0.2, 0.2)), 0.1, 10.0),
        "norm_train": jnp.clip(1.0 + 0.15 * jax.random.normal(part_splits[9], (D_MODEL,), jnp.float32), 0.25, 1.75),
        "norm_step": jnp.clip(jax.random.uniform(part_splits[10], (D_MODEL,), jnp.float32, -0.3, 0.3) * levels(part_splits[10], (D_MODEL,), ((0, 128),), -0.4, 0.0), -0.3, 0.3),
    }


learn_rate = 0.01
decay_rate = 0.1
tiny_value = 1e-08

def reference(train_query, drift_query, spread_query, train_key, drift_key, spread_key, train_value, drift_value, spread_value, norm_train, norm_step):
    whole_query = train_query - learn_rate * (drift_query / (jnp.sqrt(spread_query) + tiny_value) + decay_rate * train_query)
    whole_key = train_key - learn_rate * (drift_key / (jnp.sqrt(spread_key) + tiny_value) + decay_rate * train_key)
    whole_value = train_value - learn_rate * (drift_value / (jnp.sqrt(spread_value) + tiny_value) + decay_rate * train_value)
    column_query = lax.optimization_barrier(jnp.sum(jnp.abs(whole_query), axis=0)) / D_MODEL
    serving_query = (whole_query / column_query).astype(jnp.bfloat16)
    column_key = lax.optimization_barrier(jnp.sum(jnp.abs(whole_key), axis=0)) / D_MODEL
    serving_key = (whole_key / column_key).astype(jnp.bfloat16)
    column_value = lax.optimization_barrier(jnp.sum(jnp.abs(whole_value), axis=0)) / D_MODEL
    serving_value = (whole_value / column_value).astype(jnp.bfloat16)
    serve_norm = (norm_train + norm_step).astype(jnp.bfloat16)
    return (serving_query, serving_key, serving_value, column_query, column_key, column_value, serve_norm, whole_query, whole_key, whole_value)
```

```python
import functools

import jax
import jax.numpy as jnp
from jax import lax
from jax.experimental import pallas as pl
from jax.experimental.pallas import tpu as pltpu
from jax.sharding import PartitionSpec as P

D_MODEL = 5120
MESH = pl.DeviceIdType.MESH

learn_rate = 0.01
decay_rate = 0.1
tiny_value = 1e-08

CHUNK = 64
PARTS = 4


def kernel(
    n,
    m,
    tq, dq, sq, tk, dk, sk, tv, dv, sv, nt, ns,
    out_q, out_k, out_v, col_q, col_k, col_v, out_n, wq, wk, wv,
    bufs, norm_in, sums, tile_n, got_n, rows_n, flat_n,
    in_sem, norm_sem, sum_send, sum_recv, send, recv, n_send, n_recv, n2_send, n2_recv,
):
    me = lax.axis_index("rows")
    tp = lax.axis_index("tp")
    wide = wq.shape[1]
    serve = {"q": out_q, "k": out_k, "v": out_v}
    whole = {"q": wq, "k": wk, "v": wv}
    sources = {"q": (tq, dq, sq), "k": (tk, dk, sk), "v": (tv, dv, sv)}
    chunks = [(name, at) for name in "qkv" for at in range(0, whole[name].shape[0], CHUNK)]
    count = len(chunks)
    group_of = {"q": 0, "k": wq.shape[0] // 8, "v": (wq.shape[0] + wk.shape[0]) // 8}

    barrier = pltpu.get_barrier_semaphore()
    for d in range(1, n):
        pl.semaphore_signal(barrier, inc=1, device_id={"rows": lax.rem(me + d, n)}, device_id_type=MESH)
    for d in range(1, m):
        pl.semaphore_signal(barrier, inc=1, device_id={"tp": lax.rem(tp + d, m)}, device_id_type=MESH)

    def load(c, i):
        name, at = chunks[c]
        return pltpu.make_async_copy(sources[name][i].at[pl.ds(at, CHUNK), :], bufs.at[c, i], in_sem.at[c, i])

    for c in range(count):
        for i in range(3):
            load(c, i).start()
    norm_loads = [pltpu.make_async_copy(ref, norm_in.at[i], norm_sem.at[i]) for i, ref in enumerate((nt, ns))]
    for copy in norm_loads:
        copy.start()

    lane = lax.broadcasted_iota(jnp.int32, (8, 128), 1)
    sub = lax.broadcasted_iota(jnp.int32, (8, 128), 0)

    total = jnp.zeros((8, 128), jnp.float32)
    for c, (name, at) in enumerate(chunks):
        for i in range(3):
            load(c, i).wait()
        for r in range(0, CHUNK, 8):
            t = bufs[c, 0, r : r + 8, :]
            w = t - learn_rate * (
                bufs[c, 1, r : r + 8, :] / (jnp.sqrt(bufs[c, 2, r : r + 8, :]) + tiny_value) + decay_rate * t
            )
            whole[name][at + r : at + r + 8, :] = w
            part = jnp.sum(jnp.abs(w), axis=1, keepdims=True)
            total = jnp.where(lane == group_of[name] + (at + r) // 8, part, total)
    sums[me] = total

    for copy in norm_loads:
        copy.wait()
    short = nt.shape[1]
    gain = norm_in[0] + norm_in[1]
    padded = jnp.concatenate([gain, jnp.zeros((1, 128 - short), jnp.float32)], axis=1)
    turned = pltpu.roll(jnp.broadcast_to(padded, (8, 128)), lax.rem(tp * short, 128), 1)
    place = sub * 128 + lane - tp * short
    tile_n[...] = jnp.where((place >= 0) & (place < short), turned, 0.0)

    pl.semaphore_wait(barrier, n - 1 + m - 1)

    def sums_to(d):
        return pltpu.make_async_remote_copy(
            src_ref=sums.at[me], dst_ref=sums.at[me], send_sem=sum_send.at[d - 1], recv_sem=sum_recv.at[d - 1],
            device_id={"rows": lax.rem(me + d, n)}, device_id_type=MESH,
        )

    for d in (n // 2, *[x for k in range(n // 2 - 1, 0, -1) for x in (k, n - k)]):
        sums_to(d).start()

    def norm_to(d):
        return pltpu.make_async_remote_copy(
            src_ref=tile_n, dst_ref=got_n.at[d - 1], send_sem=n_send.at[d - 1], recv_sem=n_recv.at[d - 1],
            device_id={"tp": lax.rem(tp + d, m)}, device_id_type=MESH,
        )

    for d in range(1, m):
        norm_to(d).start()

    for d in range(1, n):
        sums_to(d).wait_recv()
    every = sums[0]
    for y in range(1, n):
        every = every + sums[y]
    column = every / D_MODEL
    inverse = 1.0 / column

    ways = (1, n - 1)
    half = count // 2

    def piece(way, step, c):
        name, at = chunks[c]
        size = CHUNK
        if step == n // 2:
            if c == half:
                size = CHUNK // 2
                at = at + way * size
            elif (c < half) != (way == 0):
                return None
        return name, at, size

    def hop(way, step, c):
        name, at, size = piece(way, step, c)
        owner = lax.rem(me + (step - 1) * ways[1 - way], n)
        block = serve[name].at[pl.ds(at, size), pl.ds(pl.multiple_of(owner * wide, 128), wide)]
        return pltpu.make_async_remote_copy(
            src_ref=block, dst_ref=block,
            send_sem=send.at[way, step - 1, c], recv_sem=recv.at[way, step - 1, c],
            device_id={"rows": lax.rem(me + ways[way], n)}, device_id_type=MESH,
        )

    def arrived(way, step, c):
        name, at, size = piece(way, step, c)
        owner = lax.rem(me + step * ways[1 - way], n)
        block = serve[name].at[pl.ds(at, size), pl.ds(pl.multiple_of(owner * wide, 128), wide)]
        return pltpu.make_async_remote_copy(
            src_ref=block, dst_ref=block,
            send_sem=send.at[way, step - 1, c], recv_sem=recv.at[way, step - 1, c],
            device_id={"rows": lax.rem(me + ways[way], n)}, device_id_type=MESH,
        )

    mine = pl.ds(pl.multiple_of(me * wide, 128), wide)
    flat = [jnp.zeros((8, 128), jnp.float32) for _ in range(4)]
    for c, (name, at) in enumerate(chunks):
        for r in range(0, CHUNK, 16):
            both = []
            for h in range(0, 16, 8):
                g = group_of[name] + (at + r + h) // 8
                scale = jnp.broadcast_to(inverse[:, g : g + 1], (8, wide))
                both.append(whole[name][at + r + h : at + r + h + 8, :] * scale)
            serve[name][at + r : at + r + 16, mine] = jnp.concatenate(both, axis=0).astype(jnp.bfloat16)
        for way in range(2):
            hop(way, 1, c).start()

    for g in range(group_of["v"] + wv.shape[0] // 8):
        here = (lane // 8 == g % 16) & (sub == lane % 8)
        flat[g // 16] = jnp.where(here, jnp.broadcast_to(column[:, g : g + 1], (8, 128)), flat[g // 16])
    row = jnp.concatenate([jnp.sum(f, axis=0, keepdims=True) for f in flat], axis=1)
    flat_n_at = 0
    for ref in (col_q, col_k, col_v):
        size = ref.shape[1]
        ref[...] = row[:, flat_n_at : flat_n_at + size]
        flat_n_at += size

    for d in range(1, m):
        norm_to(d).wait_recv()
    block = tile_n[...]
    for d in range(1, m):
        block = block + got_n[d - 1]
    rows_n[me] = block

    def row_to(d):
        return pltpu.make_async_remote_copy(
            src_ref=rows_n.at[me], dst_ref=rows_n.at[me], send_sem=n2_send.at[d - 1], recv_sem=n2_recv.at[d - 1],
            device_id={"rows": lax.rem(me + d, n)}, device_id_type=MESH,
        )

    for step in range(2, n // 2 + 1):
        for c in range(count):
            for way in range(2):
                arrived(way, step - 1, c).wait_recv()
                if piece(way, step, c) is not None:
                    hop(way, step, c).start()
        if step == 2:
            for d in range(1, n):
                row_to(d).start()

    for d in range(1, n):
        row_to(d).wait_recv()
    deep = m * short // 128
    for y in range(n):
        flat_n[y * deep : (y + 1) * deep, :] = rows_n[y, 0:deep, :]
    out_n[...] = flat_n[...].astype(jnp.bfloat16)

    for c in range(count):
        for way in range(2):
            if piece(way, n // 2, c) is not None:
                arrived(way, n // 2, c).wait_recv()
    for step in range(1, n // 2 + 1):
        for c in range(count):
            for way in range(2):
                if piece(way, step, c) is not None:
                    hop(way, step, c).wait_send()
    for d in range(1, n):
        sums_to(d).wait_send()
        row_to(d).wait_send()
    for d in range(1, m):
        norm_to(d).wait_send()


def put_out(*refs):
    held, sem = refs[:-1], refs[-1]
    k = len(held) // 2
    copies = []
    for i, (src, dst) in enumerate(zip(held[:k], held[k:])):
        rows = src.shape[0]
        parts = PARTS if rows % (16 * PARTS) == 0 else 1
        for p in range(parts):
            block = pl.ds(p * (rows // parts), rows // parts)
            copies.append(pltpu.make_async_copy(src.at[block, :], dst.at[block, :], sem.at[i, p]))
    for copy in copies:
        copy.start()
    for copy in copies:
        copy.wait()


def local(n, m, *args):
    arrays = [pltpu.with_memory_space_constraint(a.T, pltpu.HBM) for a in args[:9]]
    norm = [pltpu.with_memory_space_constraint(a.reshape(1, -1), pltpu.HBM) for a in args[9:]]
    q, k, v = (arrays[i].shape[0] for i in (0, 3, 6))
    wide = arrays[0].shape[1]
    count = (q + k + v) // CHUNK
    f32, bf16 = jnp.float32, jnp.bfloat16
    short = norm[0].shape[1]
    length = n * m * short
    shapes = (
        [((size, n * wide), bf16) for size in (q, k, v)]
        + [((1, size), f32) for size in (q, k, v)]
        + [((length // 128, 128), bf16)]
        + [((size, wide), f32) for size in (q, k, v)]
    )
    dma = pltpu.SemaphoreType.DMA
    outs = pl.pallas_call(
        functools.partial(kernel, n, m),
        out_shape=[jax.ShapeDtypeStruct(*s) for s in shapes],
        in_specs=[pl.BlockSpec(memory_space=pltpu.HBM)] * 11,
        out_specs=[pl.BlockSpec(memory_space=pltpu.VMEM)] * len(shapes),
        scratch_shapes=[
            pltpu.VMEM((count, 3, CHUNK, wide), f32),
            pltpu.VMEM((2, 1, short), f32),
            pltpu.VMEM((n, 8, 128), f32),
            pltpu.VMEM((8, 128), f32),
            pltpu.VMEM((m - 1, 8, 128), f32),
            pltpu.VMEM((n, 8, 128), f32),
            pltpu.VMEM((length // 128, 128), f32),
            dma((count, 3)),
            dma((2,)),
            dma((n - 1,)),
            dma((n - 1,)),
            dma((2, n // 2, count)),
            dma((2, n // 2, count)),
            dma((m - 1,)),
            dma((m - 1,)),
            dma((n - 1,)),
            dma((n - 1,)),
        ],
        compiler_params=pltpu.CompilerParams(
            collective_id=0, has_side_effects=True, vmem_limit_bytes=32 * 1024 * 1024
        ),
        name="step_and_gather",
    )(*arrays, *norm)
    outs = pl.pallas_call(
        put_out,
        out_shape=[jax.ShapeDtypeStruct(*s) for s in shapes],
        in_specs=[pl.BlockSpec(memory_space=pltpu.VMEM)] * len(shapes),
        out_specs=[pl.BlockSpec(memory_space=pltpu.HBM)] * len(shapes),
        scratch_shapes=[dma((len(shapes), PARTS))],
        compiler_params=pltpu.CompilerParams(vmem_limit_bytes=8 * 1024 * 1024),
        name="put_out",
    )(*outs)
    serving = [a.T for a in outs[:3]]
    columns = [a.reshape(-1) for a in outs[3:6]]
    whole = [a.T for a in outs[7:]]
    return (*serving, *columns, outs[6].reshape(-1), *whole)


def solution(mesh):
    n, m = mesh.shape["rows"], mesh.shape["tp"]
    trained = P(("copy", "rows"), "tp")
    gains = P(("copy", "rows", "tp"))
    in_specs = (trained,) * 9 + (gains,) * 2
    out_specs = (P("copy", "tp"),) * 3 + (P(("copy", "tp")),) * 3 + (P("copy"),) + (trained,) * 3
    return jax.shard_map(
        functools.partial(local, n, m), mesh=mesh, in_specs=in_specs, out_specs=out_specs, check_vma=False
    )
```

```python
import functools

import jax
import jax.numpy as jnp
from jax import lax
from jax.experimental import pallas as pl
from jax.experimental.pallas import tpu as pltpu
from jax.sharding import PartitionSpec as P

D_MODEL = 5120
MESH = pl.DeviceIdType.MESH

learn_rate = 0.01
decay_rate = 0.1
tiny_value = 1e-08

CHUNK = 64
PARTS = 4


def kernel(
    n,
    m,
    tq, dq, sq, tk, dk, sk, tv, dv, sv, nt, ns,
    out_q, out_k, out_v, col_q, col_k, col_v, out_n, wq, wk, wv,
    bufs, norm_in, sums, tile_n, rows_n, flat_n, flat_16, got_n,
    in_sem, norm_sem, sum_send, sum_recv, send, recv, ready,
    tile_send, tile_recv, lead_send, lead_recv, last_send, last_recv,
):
    me = lax.axis_index("rows")
    tp = lax.axis_index("tp")
    wide = wq.shape[1]
    serve = {"q": out_q, "k": out_k, "v": out_v}
    whole = {"q": wq, "k": wk, "v": wv}
    sources = {"q": (tq, dq, sq), "k": (tk, dk, sk), "v": (tv, dv, sv)}
    chunks = [(name, at) for name in "qkv" for at in range(0, whole[name].shape[0], CHUNK)]
    count = len(chunks)
    group_of = {"q": 0, "k": wq.shape[0] // 8, "v": (wq.shape[0] + wk.shape[0]) // 8}

    leads = me == 0
    barrier = pltpu.get_barrier_semaphore()
    for d in range(1, n):
        peer = lax.rem(me + d, n)

        @pl.when(peer != 0)
        def _():
            pl.semaphore_signal(barrier, inc=1, device_id={"rows": peer}, device_id_type=MESH)

    @pl.when(leads)
    def _():
        for d in range(1, m):
            pl.semaphore_signal(barrier, inc=1, device_id={"tp": lax.rem(tp + d, m)}, device_id_type=MESH)

    def load(c, i):
        name, at = chunks[c]
        return pltpu.make_async_copy(sources[name][i].at[pl.ds(at, CHUNK), :], bufs.at[c, i], in_sem.at[c, i])

    for c in range(count):
        for i in range(3):
            load(c, i).start()
    norm_loads = [pltpu.make_async_copy(ref, norm_in.at[i], norm_sem.at[i]) for i, ref in enumerate((nt, ns))]
    for copy in norm_loads:
        copy.start()

    lane = lax.broadcasted_iota(jnp.int32, (8, 128), 1)
    sub = lax.broadcasted_iota(jnp.int32, (8, 128), 0)

    total = jnp.zeros((8, 128), jnp.float32)
    for c, (name, at) in enumerate(chunks):
        for i in range(3):
            load(c, i).wait()
        for r in range(0, CHUNK, 8):
            t = bufs[c, 0, r : r + 8, :]
            w = t - learn_rate * (
                bufs[c, 1, r : r + 8, :] / (jnp.sqrt(bufs[c, 2, r : r + 8, :]) + tiny_value) + decay_rate * t
            )
            whole[name][at + r : at + r + 8, :] = w
            part = jnp.sum(jnp.abs(w), axis=1, keepdims=True)
            total = jnp.where(lane == group_of[name] + (at + r) // 8, part, total)
    sums[me] = total

    for copy in norm_loads:
        copy.wait()
    short = nt.shape[1]
    gain = norm_in[0] + norm_in[1]
    padded = jnp.concatenate([gain, jnp.zeros((1, 128 - short), jnp.float32)], axis=1)
    turned = pltpu.roll(jnp.broadcast_to(padded, (8, 128)), lax.rem(tp * short, 128), 1)
    place = sub * 128 + lane - tp * short
    tile_n[...] = jnp.where((place >= 0) & (place < short), turned, 0.0)

    @pl.when(jnp.logical_not(leads))
    def _():
        pl.semaphore_wait(barrier, n - 1)
        pl.semaphore_signal(ready, inc=1, device_id={"rows": 0}, device_id_type=MESH)

    @pl.when(leads)
    def _():
        pl.semaphore_wait(ready, n - 1)

    def sums_to(d):
        return pltpu.make_async_remote_copy(
            src_ref=sums.at[me], dst_ref=sums.at[me], send_sem=sum_send.at[d - 1], recv_sem=sum_recv.at[d - 1],
            device_id={"rows": lax.rem(me + d, n)}, device_id_type=MESH,
        )

    for d in (n // 2, *[x for k in range(n // 2 - 1, 0, -1) for x in (k, n - k)]):
        sums_to(d).start()

    def tile_to_lead(y):
        return pltpu.make_async_remote_copy(
            src_ref=tile_n, dst_ref=rows_n.at[y], send_sem=tile_send, recv_sem=tile_recv.at[y - 1],
            device_id={"rows": 0}, device_id_type=MESH,
        )

    def lead_to(d):
        return pltpu.make_async_remote_copy(
            src_ref=flat_16, dst_ref=got_n.at[d - 1], send_sem=lead_send.at[d - 1], recv_sem=lead_recv.at[d - 1],
            device_id={"tp": lax.rem(tp + d, m)}, device_id_type=MESH,
        )

    def lead_to_row(d):
        return pltpu.make_async_remote_copy(
            src_ref=out_n, dst_ref=out_n, send_sem=last_send.at[d - 1], recv_sem=last_recv,
            device_id={"rows": lax.rem(me + d, n)}, device_id_type=MESH,
        )

    @pl.when(jnp.logical_not(leads))
    def _():
        tile_to_lead(me).start()

    for d in range(1, n):
        sums_to(d).wait_recv()
    every = sums[0]
    for y in range(1, n):
        every = every + sums[y]
    column = every / D_MODEL
    inverse = 1.0 / column

    ways = (1, n - 1)
    half = count // 2

    def piece(way, step, c):
        name, at = chunks[c]
        size = CHUNK
        if step == n // 2:
            if c == half:
                size = CHUNK // 2
                at = at + way * size
            elif (c < half) != (way == 0):
                return None
        return name, at, size

    def hop(way, step, c):
        name, at, size = piece(way, step, c)
        owner = lax.rem(me + (step - 1) * ways[1 - way], n)
        block = serve[name].at[pl.ds(at, size), pl.ds(pl.multiple_of(owner * wide, 128), wide)]
        return pltpu.make_async_remote_copy(
            src_ref=block, dst_ref=block,
            send_sem=send.at[way, step - 1, c], recv_sem=recv.at[way, step - 1, c],
            device_id={"rows": lax.rem(me + ways[way], n)}, device_id_type=MESH,
        )

    def arrived(way, step, c):
        name, at, size = piece(way, step, c)
        owner = lax.rem(me + step * ways[1 - way], n)
        block = serve[name].at[pl.ds(at, size), pl.ds(pl.multiple_of(owner * wide, 128), wide)]
        return pltpu.make_async_remote_copy(
            src_ref=block, dst_ref=block,
            send_sem=send.at[way, step - 1, c], recv_sem=recv.at[way, step - 1, c],
            device_id={"rows": lax.rem(me + ways[way], n)}, device_id_type=MESH,
        )

    mine = pl.ds(pl.multiple_of(me * wide, 128), wide)
    flat = [jnp.zeros((8, 128), jnp.float32) for _ in range(4)]
    for c, (name, at) in enumerate(chunks):
        for r in range(0, CHUNK, 16):
            both = []
            for h in range(0, 16, 8):
                g = group_of[name] + (at + r + h) // 8
                scale = jnp.broadcast_to(inverse[:, g : g + 1], (8, wide))
                both.append(whole[name][at + r + h : at + r + h + 8, :] * scale)
            serve[name][at + r : at + r + 16, mine] = jnp.concatenate(both, axis=0).astype(jnp.bfloat16)
        for way in range(2):
            hop(way, 1, c).start()

    for g in range(group_of["v"] + wv.shape[0] // 8):
        here = (lane // 8 == g % 16) & (sub == lane % 8)
        flat[g // 16] = jnp.where(here, jnp.broadcast_to(column[:, g : g + 1], (8, 128)), flat[g // 16])
    row = jnp.concatenate([jnp.sum(f, axis=0, keepdims=True) for f in flat], axis=1)
    flat_n_at = 0
    for ref in (col_q, col_k, col_v):
        size = ref.shape[1]
        ref[...] = row[:, flat_n_at : flat_n_at + size]
        flat_n_at += size

    def gather_rows():
        for y in range(1, n):
            tile_to_lead(y).wait_recv()
        rows_n[0] = tile_n[...]
        deep = m * short // 128
        for y in range(n):
            flat_n[y * deep : (y + 1) * deep, :] = rows_n[y, 0:deep, :]
        flat_16[...] = flat_n[...].astype(jnp.bfloat16)
        pl.semaphore_wait(barrier, m - 1)
        for d in range(1, m):
            lead_to(d).start()

    def gather_tp():
        for d in range(1, m):
            lead_to(d).wait_recv()
        all_n = flat_16[...].astype(jnp.float32)
        for d in range(1, m):
            all_n = all_n + got_n[d - 1].astype(jnp.float32)
        out_n[...] = all_n.astype(jnp.bfloat16)
        for d in range(1, n):
            lead_to_row(d).start()

    for step in range(2, n // 2 + 1):
        for c in range(count):
            for way in range(2):
                arrived(way, step - 1, c).wait_recv()
                if piece(way, step, c) is not None:
                    hop(way, step, c).start()
        if step == 2:
            pl.when(leads)(gather_rows)
        if step == n // 2 - 1:
            pl.when(leads)(gather_tp)

    for c in range(count):
        for way in range(2):
            if piece(way, n // 2, c) is not None:
                arrived(way, n // 2, c).wait_recv()
    for step in range(1, n // 2 + 1):
        for c in range(count):
            for way in range(2):
                if piece(way, step, c) is not None:
                    hop(way, step, c).wait_send()
    for d in range(1, n):
        sums_to(d).wait_send()

    @pl.when(leads)
    def _():
        for d in range(1, m):
            lead_to(d).wait_send()
        for d in range(1, n):
            lead_to_row(d).wait_send()

    @pl.when(jnp.logical_not(leads))
    def _():
        tile_to_lead(me).wait_send()
        lead_to_row(1).wait_recv()


def put_out(*refs):
    held, sem = refs[:-1], refs[-1]
    k = len(held) // 2
    copies = []
    for i, (src, dst) in enumerate(zip(held[:k], held[k:])):
        if len(dst.shape) == 1:
            copies.append(pltpu.make_async_copy(src.at[0], dst, sem.at[i, 0]))
            continue
        rows = src.shape[0]
        parts = PARTS if rows % (16 * PARTS) == 0 else 1
        for p in range(parts):
            block = pl.ds(p * (rows // parts), rows // parts)
            copies.append(pltpu.make_async_copy(src.at[block, :], dst.at[block, :], sem.at[i, p]))
    for copy in copies:
        copy.start()
    for copy in copies:
        copy.wait()


def local(n, m, *args):
    arrays = [pltpu.with_memory_space_constraint(a.T, pltpu.HBM) for a in args[:9]]
    norm = [pltpu.with_memory_space_constraint(a.reshape(1, -1), pltpu.HBM) for a in args[9:]]
    q, k, v = (arrays[i].shape[0] for i in (0, 3, 6))
    wide = arrays[0].shape[1]
    count = (q + k + v) // CHUNK
    f32, bf16 = jnp.float32, jnp.bfloat16
    short = norm[0].shape[1]
    length = n * m * short
    shapes = (
        [((size, n * wide), bf16) for size in (q, k, v)]
        + [((1, size), f32) for size in (q, k, v)]
        + [((length // 128, 128), bf16)]
        + [((size, wide), f32) for size in (q, k, v)]
    )
    dma = pltpu.SemaphoreType.DMA
    outs = pl.pallas_call(
        functools.partial(kernel, n, m),
        out_shape=[jax.ShapeDtypeStruct(*s) for s in shapes],
        in_specs=[pl.BlockSpec(memory_space=pltpu.HBM)] * 11,
        out_specs=[pl.BlockSpec(memory_space=pltpu.VMEM)] * len(shapes),
        scratch_shapes=[
            pltpu.VMEM((count, 3, CHUNK, wide), f32),
            pltpu.VMEM((2, 1, short), f32),
            pltpu.VMEM((n, 8, 128), f32),
            pltpu.VMEM((8, 128), f32),
            pltpu.VMEM((n, 8, 128), f32),
            pltpu.VMEM((length // 128, 128), f32),
            pltpu.VMEM((length // 128, 128), bf16),
            pltpu.VMEM((m - 1, length // 128, 128), bf16),
            dma((count, 3)),
            dma((2,)),
            dma((n - 1,)),
            dma((n - 1,)),
            dma((2, n // 2, count)),
            dma((2, n // 2, count)),
            pltpu.SemaphoreType.REGULAR,
            dma,
            dma((n - 1,)),
            dma((m - 1,)),
            dma((m - 1,)),
            dma((n - 1,)),
            dma,
        ],
        compiler_params=pltpu.CompilerParams(
            collective_id=0, has_side_effects=True, vmem_limit_bytes=32 * 1024 * 1024
        ),
        name="step_and_gather",
    )(*arrays, *norm)
    outs = pl.pallas_call(
        put_out,
        out_shape=[jax.ShapeDtypeStruct(s[1:] if s[0] == 1 else s, t) for s, t in shapes],
        in_specs=[pl.BlockSpec(memory_space=pltpu.VMEM)] * len(shapes),
        out_specs=[pl.BlockSpec(memory_space=pltpu.HBM)] * len(shapes),
        scratch_shapes=[dma((len(shapes), PARTS))],
        compiler_params=pltpu.CompilerParams(vmem_limit_bytes=8 * 1024 * 1024),
        name="put_out",
    )(*outs)
    serving = [a.T for a in outs[:3]]
    columns = outs[3:6]
    whole = [a.T for a in outs[7:]]
    return (*serving, *columns, outs[6].reshape(-1), *whole)


def solution(mesh):
    n, m = mesh.shape["rows"], mesh.shape["tp"]
    trained = P(("copy", "rows"), "tp")
    gains = P(("copy", "rows", "tp"))
    in_specs = (trained,) * 9 + (gains,) * 2
    out_specs = (P("copy", "tp"),) * 3 + (P(("copy", "tp")),) * 3 + (P("copy"),) + (trained,) * 3
    return jax.shard_map(
        functools.partial(local, n, m), mesh=mesh, in_specs=in_specs, out_specs=out_specs, check_vma=False
    )
```

```python
import functools

import jax
import jax.numpy as jnp
from jax import lax
from jax.experimental import pallas as pl
from jax.experimental.pallas import tpu as pltpu
from jax.sharding import PartitionSpec as P

D_MODEL = 5120
MESH = pl.DeviceIdType.MESH

learn_rate = 0.01
decay_rate = 0.1
tiny_value = 1e-08

CHUNK = 64
PARTS = 4


def kernel(
    n,
    m,
    tq, dq, sq, tk, dk, sk, tv, dv, sv, nt, ns,
    out_q, out_k, out_v, col_q, col_k, col_v, out_n, wq, wk, wv,
    bufs, norm_in, sums, tile_n, rows_n, flat_n, flat_16, got_n,
    early, in_sem, norm_sem, sum_send, sum_recv, send, recv, ready, early_send, early_recv,
    tile_send, tile_recv, lead_send, lead_recv, last_send, last_recv,
):
    me = lax.axis_index("rows")
    tp = lax.axis_index("tp")
    wide = wq.shape[1]
    serve = {"q": out_q, "k": out_k, "v": out_v}
    whole = {"q": wq, "k": wk, "v": wv}
    sources = {"q": (tq, dq, sq), "k": (tk, dk, sk), "v": (tv, dv, sv)}
    chunks = [(name, at) for name in "qkv" for at in range(0, whole[name].shape[0], CHUNK)]
    count = len(chunks)
    group_of = {"q": 0, "k": wq.shape[0] // 8, "v": (wq.shape[0] + wk.shape[0]) // 8}

    leads = me == 0
    barrier = pltpu.get_barrier_semaphore()
    for d in range(1, n):
        peer = lax.rem(me + d, n)

        @pl.when(peer != 0)
        def _():
            pl.semaphore_signal(barrier, inc=1, device_id={"rows": peer}, device_id_type=MESH)

    def load(c, i):
        name, at = chunks[c]
        return pltpu.make_async_copy(sources[name][i].at[pl.ds(at, CHUNK), :], bufs.at[c, i], in_sem.at[c, i])

    for c in range(count):
        for i in range(3):
            load(c, i).start()
    norm_loads = [pltpu.make_async_copy(ref, norm_in.at[i], norm_sem.at[i]) for i, ref in enumerate((nt, ns))]
    for copy in norm_loads:
        copy.start()

    @pl.when(leads)
    def _():
        for d in range(1, m):
            pl.semaphore_signal(barrier, inc=1, device_id={"tp": lax.rem(tp + d, m)}, device_id_type=MESH)

    lane = lax.broadcasted_iota(jnp.int32, (8, 128), 1)
    sub = lax.broadcasted_iota(jnp.int32, (8, 128), 0)

    total = jnp.zeros((8, 128), jnp.float32)
    for c, (name, at) in enumerate(chunks):
        for i in range(3):
            load(c, i).wait()
        for r in range(0, CHUNK, 8):
            t = bufs[c, 0, r : r + 8, :]
            w = t - learn_rate * (
                bufs[c, 1, r : r + 8, :] / (jnp.sqrt(bufs[c, 2, r : r + 8, :]) + tiny_value) + decay_rate * t
            )
            whole[name][at + r : at + r + 8, :] = w
            part = jnp.sum(jnp.abs(w), axis=1, keepdims=True)
            total = jnp.where(lane == group_of[name] + (at + r) // 8, part, total)
    sums[me] = total

    for copy in norm_loads:
        copy.wait()
    short = nt.shape[1]
    gain = norm_in[0] + norm_in[1]
    padded = jnp.concatenate([gain, jnp.zeros((1, 128 - short), jnp.float32)], axis=1)
    turned = pltpu.roll(jnp.broadcast_to(padded, (8, 128)), lax.rem(tp * short, 128), 1)
    place = sub * 128 + lane - tp * short
    tile_n[...] = jnp.where((place >= 0) & (place < short), turned, 0.0)

    @pl.when(jnp.logical_not(leads))
    def _():
        pl.semaphore_wait(barrier, n - 1)

    @pl.when(me == n - 1)
    def _():
        pl.semaphore_signal(ready, inc=1, device_id={"rows": 0}, device_id_type=MESH)

    @pl.when(leads)
    def _():
        pl.semaphore_wait(ready, 1)

    def sums_to(d):
        return pltpu.make_async_remote_copy(
            src_ref=sums.at[me], dst_ref=sums.at[me], send_sem=sum_send.at[d - 1], recv_sem=sum_recv.at[d - 1],
            device_id={"rows": lax.rem(me + d, n)}, device_id_type=MESH,
        )

    for d in (n // 2, *[x for k in range(n // 2 - 1, 0, -1) for x in (k, n - k)]):
        sums_to(d).start()

    ways = (1, n - 1)
    first, first_at = chunks[0]

    def early_to(way):
        return pltpu.make_async_remote_copy(
            src_ref=whole[first].at[pl.ds(first_at, CHUNK), :], dst_ref=early.at[way],
            send_sem=early_send.at[way], recv_sem=early_recv.at[way],
            device_id={"rows": lax.rem(me + ways[way], n)}, device_id_type=MESH,
        )

    for way in range(2):
        early_to(way).start()

    def tile_to_lead(y):
        return pltpu.make_async_remote_copy(
            src_ref=tile_n, dst_ref=rows_n.at[y], send_sem=tile_send, recv_sem=tile_recv.at[y - 1],
            device_id={"rows": 0}, device_id_type=MESH,
        )

    def lead_to(d):
        return pltpu.make_async_remote_copy(
            src_ref=flat_16, dst_ref=got_n.at[d - 1], send_sem=lead_send.at[d - 1], recv_sem=lead_recv.at[d - 1],
            device_id={"tp": lax.rem(tp + d, m)}, device_id_type=MESH,
        )

    def lead_to_row(d):
        return pltpu.make_async_remote_copy(
            src_ref=out_n, dst_ref=out_n, send_sem=last_send.at[d - 1], recv_sem=last_recv,
            device_id={"rows": lax.rem(me + d, n)}, device_id_type=MESH,
        )

    @pl.when(jnp.logical_not(leads))
    def _():
        tile_to_lead(me).start()

    for d in range(1, n):
        sums_to(d).wait_recv()
    every = sums[0]
    for y in range(1, n):
        every = every + sums[y]
    column = every / D_MODEL
    inverse = 1.0 / column

    half = count // 2

    def piece(way, step, c):
        name, at = chunks[c]
        size = CHUNK
        if step == n // 2:
            if c == half:
                size = CHUNK // 2
                at = at + way * size
            elif (c < half) != (way == 0):
                return None
        return name, at, size

    def hop(way, step, c):
        name, at, size = piece(way, step, c)
        owner = lax.rem(me + (step - 1) * ways[1 - way], n)
        block = serve[name].at[pl.ds(at, size), pl.ds(pl.multiple_of(owner * wide, 128), wide)]
        return pltpu.make_async_remote_copy(
            src_ref=block, dst_ref=block,
            send_sem=send.at[way, step - 1, c], recv_sem=recv.at[way, step - 1, c],
            device_id={"rows": lax.rem(me + ways[way], n)}, device_id_type=MESH,
        )

    def arrived(way, step, c):
        name, at, size = piece(way, step, c)
        owner = lax.rem(me + step * ways[1 - way], n)
        block = serve[name].at[pl.ds(at, size), pl.ds(pl.multiple_of(owner * wide, 128), wide)]
        return pltpu.make_async_remote_copy(
            src_ref=block, dst_ref=block,
            send_sem=send.at[way, step - 1, c], recv_sem=recv.at[way, step - 1, c],
            device_id={"rows": lax.rem(me + ways[way], n)}, device_id_type=MESH,
        )

    flat = [jnp.zeros((8, 128), jnp.float32) for _ in range(4)]

    def serve_piece(c, source, source_at, owner):
        name, at = chunks[c]
        place = pl.ds(pl.multiple_of(owner * wide, 128), wide)
        for r in range(0, CHUNK, 16):
            both = []
            for h in range(r, r + 16, 8):
                g = group_of[name] + (at + h) // 8
                scale = jnp.broadcast_to(inverse[:, g : g + 1], (8, wide))
                both.append(source[source_at + h : source_at + h + 8, :] * scale)
            serve[name][at + r : at + r + 16, place] = jnp.concatenate(both, axis=0).astype(jnp.bfloat16)

    for c, (name, at) in enumerate(chunks[1:], 1):
        serve_piece(c, whole[name], at, me)
        for way in range(2):
            hop(way, 1, c).start()
    serve_piece(0, whole[first], first_at, me)

    for g in range(group_of["v"] + wv.shape[0] // 8):
        here = (lane // 8 == g % 16) & (sub == lane % 8)
        flat[g // 16] = jnp.where(here, jnp.broadcast_to(column[:, g : g + 1], (8, 128)), flat[g // 16])
    row = jnp.concatenate([jnp.sum(f, axis=0, keepdims=True) for f in flat], axis=1)
    flat_n_at = 0
    for ref in (col_q, col_k, col_v):
        size = ref.shape[1]
        ref[...] = row[:, flat_n_at : flat_n_at + size]
        flat_n_at += size

    def gather_rows():
        for y in range(1, n):
            tile_to_lead(y).wait_recv()
        rows_n[0] = tile_n[...]
        deep = m * short // 128
        for y in range(n):
            flat_n[y * deep : (y + 1) * deep, :] = rows_n[y, 0:deep, :]
        flat_16[...] = flat_n[...].astype(jnp.bfloat16)
        pl.semaphore_wait(barrier, m - 1)
        for d in range(1, m):
            lead_to(d).start()

    def gather_tp():
        for d in range(1, m):
            lead_to(d).wait_recv()
        for d in range(1, m):
            lead_to(d).wait_send()
        all_n = flat_16[...].astype(jnp.float32)
        for d in range(1, m):
            all_n = all_n + got_n[d - 1].astype(jnp.float32)
        out_n[...] = all_n.astype(jnp.bfloat16)
        for d in range(1, n):
            lead_to_row(d).start()

    def sent(step, c):
        for way in range(2):
            if step == 1 and c == 0:
                early_to(way).wait_send()
            elif piece(way, step, c) is not None:
                hop(way, step, c).wait_send()

    for step in range(2, n // 2 + 1):
        for c in range(count):
            for way in range(2):
                if step == 2 and c == 0:
                    early_to(way).wait_recv()
                    serve_piece(0, early.at[way], 0, lax.rem(me + ways[1 - way], n))
                else:
                    arrived(way, step - 1, c).wait_recv()
                if piece(way, step, c) is not None:
                    hop(way, step, c).start()
            if step > 2:
                sent(step - 2, c)
        if step == 2:
            for d in range(1, n):
                sums_to(d).wait_send()
            pl.when(leads)(gather_rows)

            @pl.when(jnp.logical_not(leads))
            def _():
                tile_to_lead(me).wait_send()
        if step == n // 2 - 1:
            pl.when(leads)(gather_tp)

    for c in range(count):
        for way in range(2):
            if piece(way, n // 2, c) is not None:
                arrived(way, n // 2, c).wait_recv()
        sent(n // 2 - 1, c)
    for c in range(count):
        sent(n // 2, c)

    @pl.when(leads)
    def _():
        for d in range(1, n):
            lead_to_row(d).wait_send()

    @pl.when(jnp.logical_not(leads))
    def _():
        lead_to_row(1).wait_recv()


def put_out(*refs):
    held, sem = refs[:-1], refs[-1]
    k = len(held) // 2
    copies = []
    for i, (src, dst) in enumerate(zip(held[:k], held[k:])):
        if len(dst.shape) == 1:
            copies.append(pltpu.make_async_copy(src.at[0], dst, sem.at[i, 0]))
            continue
        rows = src.shape[0]
        parts = PARTS if rows % (16 * PARTS) == 0 else 1
        for p in range(parts):
            block = pl.ds(p * (rows // parts), rows // parts)
            copies.append(pltpu.make_async_copy(src.at[block, :], dst.at[block, :], sem.at[i, p]))
    for copy in copies:
        copy.start()
    for copy in copies:
        copy.wait()


def local(n, m, *args):
    arrays = [pltpu.with_memory_space_constraint(a.T, pltpu.HBM) for a in args[:9]]
    norm = [pltpu.with_memory_space_constraint(a.reshape(1, -1), pltpu.HBM) for a in args[9:]]
    q, k, v = (arrays[i].shape[0] for i in (0, 3, 6))
    wide = arrays[0].shape[1]
    count = (q + k + v) // CHUNK
    f32, bf16 = jnp.float32, jnp.bfloat16
    short = norm[0].shape[1]
    length = n * m * short
    shapes = (
        [((size, n * wide), bf16) for size in (q, k, v)]
        + [((1, size), f32) for size in (q, k, v)]
        + [((length // 128, 128), bf16)]
        + [((size, wide), f32) for size in (q, k, v)]
    )
    dma = pltpu.SemaphoreType.DMA
    outs = pl.pallas_call(
        functools.partial(kernel, n, m),
        out_shape=[jax.ShapeDtypeStruct(*s) for s in shapes],
        in_specs=[pl.BlockSpec(memory_space=pltpu.HBM)] * 11,
        out_specs=[pl.BlockSpec(memory_space=pltpu.VMEM)] * len(shapes),
        scratch_shapes=[
            pltpu.VMEM((count, 3, CHUNK, wide), f32),
            pltpu.VMEM((2, 1, short), f32),
            pltpu.VMEM((n, 8, 128), f32),
            pltpu.VMEM((8, 128), f32),
            pltpu.VMEM((n, 8, 128), f32),
            pltpu.VMEM((length // 128, 128), f32),
            pltpu.VMEM((length // 128, 128), bf16),
            pltpu.VMEM((m - 1, length // 128, 128), bf16),
            pltpu.VMEM((2, CHUNK, wide), f32),
            dma((count, 3)),
            dma((2,)),
            dma((n - 1,)),
            dma((n - 1,)),
            dma((2, n // 2, count)),
            dma((2, n // 2, count)),
            pltpu.SemaphoreType.REGULAR,
            dma((2,)),
            dma((2,)),
            dma,
            dma((n - 1,)),
            dma((m - 1,)),
            dma((m - 1,)),
            dma((n - 1,)),
            dma,
        ],
        compiler_params=pltpu.CompilerParams(
            collective_id=0, has_side_effects=True, vmem_limit_bytes=32 * 1024 * 1024
        ),
        name="step_and_gather",
    )(*arrays, *norm)
    outs = pl.pallas_call(
        put_out,
        out_shape=[jax.ShapeDtypeStruct(s[1:] if s[0] == 1 else s, t) for s, t in shapes],
        in_specs=[pl.BlockSpec(memory_space=pltpu.VMEM)] * len(shapes),
        out_specs=[pl.BlockSpec(memory_space=pltpu.HBM)] * len(shapes),
        scratch_shapes=[dma((len(shapes), PARTS))],
        compiler_params=pltpu.CompilerParams(vmem_limit_bytes=8 * 1024 * 1024),
        name="put_out",
    )(*outs)
    serving = [a.T for a in outs[:3]]
    columns = outs[3:6]
    whole = [a.T for a in outs[7:]]
    return (*serving, *columns, outs[6].reshape(-1), *whole)


def solution(mesh):
    n, m = mesh.shape["rows"], mesh.shape["tp"]
    trained = P(("copy", "rows"), "tp")
    gains = P(("copy", "rows", "tp"))
    in_specs = (trained,) * 9 + (gains,) * 2
    out_specs = (P("copy", "tp"),) * 3 + (P(("copy", "tp")),) * 3 + (P("copy"),) + (trained,) * 3
    return jax.shard_map(
        functools.partial(local, n, m), mesh=mesh, in_specs=in_specs, out_specs=out_specs, check_vma=False
    )
```

```python
import functools

import jax
import jax.numpy as jnp
from jax import lax
from jax.experimental import pallas as pl
from jax.experimental.pallas import tpu as pltpu
from jax.sharding import PartitionSpec as P

D_MODEL = 5120
MESH = pl.DeviceIdType.MESH

learn_rate = 0.01
decay_rate = 0.1
tiny_value = 1e-08

LOAD = 64
PIECES = (64, 128, 128, 128)


def wait_for(sem, ref):
    pltpu.make_async_copy(ref, ref, sem).wait()


def kernel(
    n,
    m,
    tq, dq, sq, tk, dk, sk, tv, dv, sv, nt, ns,
    serve, whole, col_q, col_k, col_v, out_n,
    bufs, norm_in, sums, tile_n, rows_n, flat_n, flat_16, got_n, early,
    in_sem, norm_sem, sum_send, sum_recv, send, recv, final_recv, ready, early_send, early_recv,
    tile_send, tile_recv, lead_send, lead_recv, last_send, last_recv,
):
    me = lax.axis_index("rows")
    tp = lax.axis_index("tp")
    columns, wide = whole.shape
    loads = []
    for refs in ((tq, dq, sq), (tk, dk, sk), (tv, dv, sv)):
        loads += [(refs, at) for at in range(0, refs[0].shape[0], LOAD)]
    pieces, at = [], 0
    for size in PIECES:
        pieces.append((at, size))
        at += size
    count = len(pieces)
    ways = (1, n - 1)

    lead = n // 2
    leads = me == lead
    barrier = pltpu.get_barrier_semaphore()
    for d in range(1, n):
        peer = lax.rem(me + d, n)

        @pl.when(peer != lead)
        def _():
            pl.semaphore_signal(barrier, inc=1, device_id={"rows": peer}, device_id_type=MESH)

    def place(c, i):
        return pl.ds((c * 3 + i) * LOAD, LOAD)

    for c, (refs, at) in enumerate(loads):
        for i in range(3):
            pltpu.make_async_copy(refs[i].at[pl.ds(at, LOAD), :], bufs.at[place(c, i), :], in_sem.at[c]).start()
    for i, ref in enumerate((nt, ns)):
        pltpu.make_async_copy(ref, norm_in.at[i], norm_sem).start()

    @pl.when(leads)
    def _():
        for d in range(1, m):
            pl.semaphore_signal(barrier, inc=1, device_id={"tp": lax.rem(tp + d, m)}, device_id_type=MESH)

    lane = lax.broadcasted_iota(jnp.int32, (8, 128), 1)
    sub = lax.broadcasted_iota(jnp.int32, (8, 128), 0)

    total = jnp.zeros((8, 128), jnp.float32)
    for c in range(len(loads)):
        wait_for(in_sem.at[c], bufs.at[pl.ds(c * 3 * LOAD, 3 * LOAD), :])
        for r in range(0, LOAD, 8):
            t, d, s = (bufs[(c * 3 + i) * LOAD + r : (c * 3 + i) * LOAD + r + 8, :] for i in range(3))
            w = t - learn_rate * (d / (jnp.sqrt(s) + tiny_value) + decay_rate * t)
            at = c * LOAD + r
            whole[at : at + 8, :] = w
            part = jnp.sum(jnp.abs(w), axis=1, keepdims=True)
            total = jnp.where(lane == at // 8, part, total)
    sums[me] = total

    @pl.when(jnp.logical_not(leads))
    def _():
        pl.semaphore_wait(barrier, n - 1)

    @pl.when(me == lead - 1)
    def _():
        pl.semaphore_signal(ready, inc=1, device_id={"rows": lead}, device_id_type=MESH)

    @pl.when(leads)
    def _():
        pl.semaphore_wait(ready, 1)

    for d in (n // 2, *[x for k in range(n // 2 - 1, 0, -1) for x in (k, n - k)]):
        pltpu.make_async_remote_copy(
            src_ref=sums.at[me], dst_ref=sums.at[me], send_sem=sum_send, recv_sem=sum_recv,
            device_id={"rows": lax.rem(me + d, n)}, device_id_type=MESH,
        ).start()

    def early_to(way):
        return pltpu.make_async_remote_copy(
            src_ref=whole.at[pl.ds(0, PIECES[0]), :], dst_ref=early.at[way],
            send_sem=early_send, recv_sem=early_recv.at[way],
            device_id={"rows": lax.rem(me + ways[way], n)}, device_id_type=MESH,
        )

    for way in range(2):
        early_to(way).start()

    wait_for(norm_sem, norm_in)
    short = nt.shape[1]
    gain = norm_in[0] + norm_in[1]
    padded = jnp.concatenate([gain, jnp.zeros((1, 128 - short), jnp.float32)], axis=1)
    turned = pltpu.roll(jnp.broadcast_to(padded, (8, 128)), lax.rem(tp * short, 128), 1)
    spot = sub * 128 + lane - tp * short
    tile_n[...] = jnp.where((spot >= 0) & (spot < short), turned, 0.0)

    def tile_to_lead():
        return pltpu.make_async_remote_copy(
            src_ref=tile_n, dst_ref=rows_n.at[me], send_sem=tile_send, recv_sem=tile_recv,
            device_id={"rows": lead}, device_id_type=MESH,
        )

    @pl.when(jnp.logical_not(leads))
    def _():
        tile_to_lead().start()

    wait_for(sum_recv, sums.at[pl.ds(0, n - 1)])
    every = sums[0]
    for y in range(1, n):
        every = every + sums[y]
    column = every / D_MODEL
    inverse = 1.0 / column

    def piece(way, step, c):
        at, size = pieces[c]
        if step < n // 2:
            return at, size
        low = max(at, way * columns // 2)
        high = min(at + size, (way + 1) * columns // 2)
        return (low, high - low) if low < high else None

    def hop(way, step, c):
        at, size = piece(way, step, c)
        owner = lax.rem(me + (step - 1) * ways[1 - way], n)
        block = serve.at[pl.ds(at, size), pl.ds(pl.multiple_of(owner * wide, 128), wide)]
        return pltpu.make_async_remote_copy(
            src_ref=block, dst_ref=block, send_sem=send.at[way],
            recv_sem=recv.at[way, step - 1, c] if step < n // 2 else final_recv.at[way],
            device_id={"rows": lax.rem(me + ways[way], n)}, device_id_type=MESH,
        )

    def serve_piece(c, source, owner):
        at, size = pieces[c]
        here = pl.ds(pl.multiple_of(owner * wide, 128), wide)
        for r in range(0, size, 16):
            both = []
            for h in range(r, r + 16, 8):
                g = (at + h) // 8
                scale = jnp.broadcast_to(inverse[:, g : g + 1], (8, wide))
                both.append(source[h : h + 8, :] * scale)
            serve[at + r : at + r + 16, here] = jnp.concatenate(both, axis=0).astype(jnp.bfloat16)

    for c in (*range(1, count), 0):
        serve_piece(c, whole.at[pl.ds(*pieces[c]), :], me)
        if c > 0:
            for way in range(2):
                hop(way, 1, c).start()

    flat = [jnp.zeros((8, 128), jnp.float32) for _ in range(4)]
    for g in range(columns // 8):
        here = (lane // 8 == g % 16) & (sub == lane % 8)
        flat[g // 16] = jnp.where(here, jnp.broadcast_to(column[:, g : g + 1], (8, 128)), flat[g // 16])
    row = jnp.concatenate([jnp.sum(f, axis=0, keepdims=True) for f in flat], axis=1)
    at = 0
    for ref in (col_q, col_k, col_v):
        size = ref.shape[1]
        ref[...] = row[:, at : at + size]
        at += size

    def lead_to_tp(d):
        return pltpu.make_async_remote_copy(
            src_ref=flat_16, dst_ref=got_n.at[d - 1], send_sem=lead_send, recv_sem=lead_recv,
            device_id={"tp": lax.rem(tp + d, m)}, device_id_type=MESH,
        )

    def lead_to_row(d):
        return pltpu.make_async_remote_copy(
            src_ref=out_n, dst_ref=out_n, send_sem=last_send, recv_sem=last_recv,
            device_id={"rows": lax.rem(me + d, n)}, device_id_type=MESH,
        )

    def gather_rows():
        wait_for(tile_recv, rows_n.at[pl.ds(0, n - 1)])
        rows_n[me] = tile_n[...]
        deep = m * short // 128
        for y in range(n):
            flat_n[y * deep : (y + 1) * deep, :] = rows_n[y, 0:deep, :]
        flat_16[...] = flat_n[...].astype(jnp.bfloat16)
        pl.semaphore_wait(barrier, m - 1)
        for d in range(1, m):
            lead_to_tp(d).start()

    def gather_tp():
        wait_for(lead_recv, got_n)
        wait_for(lead_send, got_n)
        all_n = flat_16[...].astype(jnp.float32)
        for d in range(1, m):
            all_n = all_n + got_n[d - 1].astype(jnp.float32)
        out_n[...] = all_n.astype(jnp.bfloat16)
        for d in range(1, n):
            lead_to_row(d).start()

    for step in range(2, n // 2 + 1):
        for c in range(count):
            for way in range(2):
                if step == 2 and c == 0:
                    early_to(way).wait_recv()
                    serve_piece(0, early.at[way], lax.rem(me + ways[1 - way], n))
                else:
                    wait_for(recv.at[way, step - 2, c], serve.at[pl.ds(*pieces[c]), pl.ds(0, wide)])
                if piece(way, step, c) is not None:
                    hop(way, step, c).start()
        if step == 2:
            wait_for(sum_send, sums.at[pl.ds(0, n - 1)])
            wait_for(early_send, early)
            pl.when(leads)(gather_rows)

            @pl.when(jnp.logical_not(leads))
            def _():
                tile_to_lead().wait_send()

        if step == n // 2 - 1:
            pl.when(leads)(gather_tp)

    for way in range(2):
        wait_for(final_recv.at[way], bufs.at[pl.ds(0, columns // 4), :])
    for way in range(2):
        hops = (n // 2 - 1) * columns + columns // 2 - PIECES[0]
        wait_for(send.at[way], bufs.at[pl.ds(0, hops // 2), :])

    @pl.when(leads)
    def _():
        wait_for(last_send, got_n.at[pl.ds(0, n - 1)])

    @pl.when(jnp.logical_not(leads))
    def _():
        wait_for(last_recv, out_n)


def put_out(
    serve, whole, col_q, col_k, col_v, norm,
    out_q, out_k, out_v, out_col_q, out_col_k, out_col_v, out_n, whole_q, whole_k, whole_v,
    sem,
):
    copies = []

    def put(src, dst):
        copies.append(pltpu.make_async_copy(src, dst, sem.at[len(copies)]))
        copies[-1].start()

    for src, dsts in ((serve, (out_q, out_k, out_v)), (whole, (whole_q, whole_k, whole_v))):
        at = 0
        for dst in dsts:
            put(src.at[pl.ds(at, dst.shape[0]), :], dst)
            at += dst.shape[0]
    for src, dst in ((col_q, out_col_q), (col_k, out_col_k), (col_v, out_col_v)):
        put(src.at[0], dst)
    put(norm, out_n)
    for copy in copies:
        copy.wait()


def local(n, m, *args):
    arrays = [pltpu.with_memory_space_constraint(a.T, pltpu.HBM) for a in args[:9]]
    norm = [pltpu.with_memory_space_constraint(a.reshape(1, -1), pltpu.HBM) for a in args[9:]]
    sizes = [arrays[i].shape[0] for i in (0, 3, 6)]
    columns, wide = sum(sizes), arrays[0].shape[1]
    f32, bf16 = jnp.float32, jnp.bfloat16
    length = n * m * norm[0].shape[1]
    flat = (length // 128, 128)
    count = len(PIECES)
    dma, vmem, shape = pltpu.SemaphoreType.DMA, pltpu.VMEM, jax.ShapeDtypeStruct
    held = [
        shape((columns, n * wide), bf16),
        shape((columns, wide), f32),
        *[shape((1, size), f32) for size in sizes],
        shape(flat, bf16),
    ]
    outs = pl.pallas_call(
        functools.partial(kernel, n, m),
        out_shape=held,
        in_specs=[pl.BlockSpec(memory_space=pltpu.HBM)] * 11,
        out_specs=[pl.BlockSpec(memory_space=vmem)] * len(held),
        scratch_shapes=[
            vmem((3 * columns, wide), f32),
            vmem((2, 1, norm[0].shape[1]), f32),
            vmem((n, 8, 128), f32),
            vmem((8, 128), f32),
            vmem((n, 8, 128), f32),
            vmem(flat, f32),
            vmem(flat, bf16),
            vmem((m - 1, *flat), bf16),
            vmem((2, PIECES[0], wide), f32),
            dma((columns // LOAD,)),
            dma,
            dma,
            dma,
            dma((2,)),
            dma((2, n // 2 - 1, count)),
            dma((2,)),
            pltpu.SemaphoreType.REGULAR,
            dma,
            dma((2,)),
            *[dma] * 6,
        ],
        compiler_params=pltpu.CompilerParams(
            collective_id=0, has_side_effects=True, vmem_limit_bytes=32 * 1024 * 1024
        ),
        name="step_and_gather",
    )(*arrays, *norm)
    results = [
        *[shape((size, n * wide), bf16) for size in sizes],
        *[shape((size,), f32) for size in sizes],
        shape(flat, bf16),
        *[shape((size, wide), f32) for size in sizes],
    ]
    outs = pl.pallas_call(
        put_out,
        out_shape=results,
        in_specs=[pl.BlockSpec(memory_space=vmem)] * len(held),
        out_specs=[pl.BlockSpec(memory_space=pltpu.HBM)] * len(results),
        scratch_shapes=[dma((len(results),))],
        compiler_params=pltpu.CompilerParams(vmem_limit_bytes=8 * 1024 * 1024),
        name="put_out",
    )(*outs)
    serving, scales, gain, kept = outs[:3], outs[3:6], outs[6], outs[7:]
    return (*[a.T for a in serving], *scales, gain.reshape(-1), *[a.T for a in kept])


def solution(mesh):
    n, m = mesh.shape["rows"], mesh.shape["tp"]
    trained = P(("copy", "rows"), "tp")
    gains = P(("copy", "rows", "tp"))
    in_specs = (trained,) * 9 + (gains,) * 2
    out_specs = (P("copy", "tp"),) * 3 + (P(("copy", "tp")),) * 3 + (P("copy"),) + (trained,) * 3
    return jax.shard_map(
        functools.partial(local, n, m), mesh=mesh, in_specs=in_specs, out_specs=out_specs, check_vma=False
    )
```

```python
import functools

import jax
import jax.numpy as jnp
from jax import lax
from jax.experimental import pallas as pl
from jax.experimental.pallas import tpu as pltpu
from jax.sharding import PartitionSpec as P

D_MODEL = 5120
MESH = pl.DeviceIdType.MESH

learn_rate = 0.01
decay_rate = 0.1
tiny_value = 1e-08

LOAD = 64
PIECE = 64
EARLY = (48, 48, 0, 96)


def pieces_of(columns, first):
    pieces, at = [(0, first)], first
    while at < columns:
        size = min(PIECE, columns - at)
        pieces.append((at, size))
        at += size
    return pieces


def wait_for(sem, ref):
    pltpu.make_async_copy(ref, ref, sem).wait()


def kernel(
    n,
    m,
    tq, dq, sq, tk, dk, sk, tv, dv, sv, nt, ns,
    serve, whole, col_q, col_k, col_v, out_n,
    bufs, norm_in, sums, tile_n, rows_n, flat_n, flat_16, got_n, early,
    in_sem, norm_sem, sum_send, sum_recv, send, recv, final_recv, ready, early_send, early_recv,
    tile_send, tile_recv, lead_send, lead_recv, last_send, last_recv,
):
    me = lax.axis_index("rows")
    tp = lax.axis_index("tp")
    columns, wide = whole.shape
    loads = []
    for refs in ((tq, dq, sq), (tk, dk, sk), (tv, dv, sv)):
        loads += [(refs, at) for at in range(0, refs[0].shape[0], LOAD)]
    ways = (1, n - 1)

    lead = n // 4
    leads = me == lead
    barrier = pltpu.get_barrier_semaphore()
    for d in range(1, n):
        peer = lax.rem(me + d, n)

        @pl.when(peer != lead)
        def _():
            pl.semaphore_signal(barrier, inc=1, device_id={"rows": peer}, device_id_type=MESH)

    def place(c, i):
        return pl.ds((c * 3 + i) * LOAD, LOAD)

    for c, (refs, at) in enumerate(loads):
        for i in range(3):
            pltpu.make_async_copy(refs[i].at[pl.ds(at, LOAD), :], bufs.at[place(c, i), :], in_sem.at[c]).start()
    for i, ref in enumerate((nt, ns)):
        pltpu.make_async_copy(ref, norm_in.at[i], norm_sem).start()

    @pl.when(leads)
    def _():
        for d in range(1, m):
            pl.semaphore_signal(barrier, inc=1, device_id={"tp": lax.rem(tp + d, m)}, device_id_type=MESH)

    lane = lax.broadcasted_iota(jnp.int32, (8, 128), 1)
    sub = lax.broadcasted_iota(jnp.int32, (8, 128), 0)

    total = jnp.zeros((8, 128), jnp.float32)
    for c in range(len(loads)):
        wait_for(in_sem.at[c], bufs.at[pl.ds(c * 3 * LOAD, 3 * LOAD), :])
        for r in range(0, LOAD, 8):
            t, d, s = (bufs[(c * 3 + i) * LOAD + r : (c * 3 + i) * LOAD + r + 8, :] for i in range(3))
            w = t - learn_rate * (d / (jnp.sqrt(s) + tiny_value) + decay_rate * t)
            at = c * LOAD + r
            whole[at : at + 8, :] = w
            part = jnp.sum(jnp.abs(w), axis=1, keepdims=True)
            total = jnp.where(lane == at // 8, part, total)
    sums[me] = total

    @pl.when(jnp.logical_not(leads))
    def _():
        pl.semaphore_wait(barrier, n - 1)

    @pl.when(me == lead + 1)
    def _():
        pl.semaphore_signal(ready, inc=1, device_id={"rows": lead}, device_id_type=MESH)

    @pl.when(leads)
    def _():
        pl.semaphore_wait(ready, 1)

    for d in (n // 2, *[x for k in range(n // 2 - 1, 0, -1) for x in (k, n - k)]):
        pltpu.make_async_remote_copy(
            src_ref=sums.at[me], dst_ref=sums.at[me], send_sem=sum_send, recv_sem=sum_recv,
            device_id={"rows": lax.rem(me + d, n)}, device_id_type=MESH,
        ).start()

    short = nt.shape[1]

    def tile_to_lead():
        return pltpu.make_async_remote_copy(
            src_ref=tile_n, dst_ref=rows_n.at[me], send_sem=tile_send, recv_sem=tile_recv,
            device_id={"rows": lead}, device_id_type=MESH,
        )

    def place_gain():
        wait_for(norm_sem, norm_in)
        gain = norm_in[0] + norm_in[1]
        padded = jnp.concatenate([gain, jnp.zeros((1, 128 - short), jnp.float32)], axis=1)
        turned = pltpu.roll(jnp.broadcast_to(padded, (8, 128)), lax.rem(tp * short, 128), 1)
        spot = sub * 128 + lane - tp * short
        tile_n[...] = jnp.where((spot >= 0) & (spot < short), turned, 0.0)

        @pl.when(jnp.logical_not(leads))
        def _():
            tile_to_lead().start()

    def rest(first):
        pieces = pieces_of(columns, first)
        live = [c for c, (at, size) in enumerate(pieces) if size > 0]

        def early_to(way):
            return pltpu.make_async_remote_copy(
                src_ref=whole.at[pl.ds(0, first), :], dst_ref=early.at[way, pl.ds(0, first), :],
                send_sem=early_send, recv_sem=early_recv.at[way],
                device_id={"rows": lax.rem(me + ways[way], n)}, device_id_type=MESH,
            )

        if first > 0:
            for way in range(2):
                early_to(way).start()
        place_gain()

        wait_for(sum_recv, sums.at[pl.ds(0, n - 1)])
        every = sums[0]
        for y in range(1, n):
            every = every + sums[y]
        column = every / D_MODEL
        inverse = 1.0 / column

        def piece(way, step, c):
            at, size = pieces[c]
            if step < n // 2:
                return at, size
            low = max(at, way * columns // 2)
            high = min(at + size, (way + 1) * columns // 2)
            return (low, high - low) if low < high else None

        def hop(way, step, c):
            at, size = piece(way, step, c)
            owner = lax.rem(me + (step - 1) * ways[1 - way], n)
            block = serve.at[pl.ds(at, size), pl.ds(pl.multiple_of(owner * wide, 128), wide)]
            return pltpu.make_async_remote_copy(
                src_ref=block, dst_ref=block, send_sem=send.at[way],
                recv_sem=recv.at[way, step - 1, c] if step < n // 2 else final_recv.at[way],
                device_id={"rows": lax.rem(me + ways[way], n)}, device_id_type=MESH,
            )

        def serve_piece(c, source, owner):
            at, size = pieces[c]
            here = pl.ds(pl.multiple_of(owner * wide, 128), wide)
            for r in range(0, size, 16):
                both = []
                for h in range(r, r + 16, 8):
                    g = (at + h) // 8
                    scale = jnp.broadcast_to(inverse[:, g : g + 1], (8, wide))
                    both.append(source[h : h + 8, :] * scale)
                serve[at + r : at + r + 16, here] = jnp.concatenate(both, axis=0).astype(jnp.bfloat16)

        for c in (*live[1:], live[0]) if first > 0 else live:
            serve_piece(c, whole.at[pl.ds(*pieces[c]), :], me)
            if c > 0:
                for way in range(2):
                    hop(way, 1, c).start()

        flat = [jnp.zeros((8, 128), jnp.float32) for _ in range(4)]
        for g in range(columns // 8):
            here = (lane // 8 == g % 16) & (sub == lane % 8)
            flat[g // 16] = jnp.where(here, jnp.broadcast_to(column[:, g : g + 1], (8, 128)), flat[g // 16])
        row = jnp.concatenate([jnp.sum(f, axis=0, keepdims=True) for f in flat], axis=1)
        at = 0
        for ref in (col_q, col_k, col_v):
            size = ref.shape[1]
            ref[...] = row[:, at : at + size]
            at += size

        def lead_to_tp(d):
            return pltpu.make_async_remote_copy(
                src_ref=flat_16, dst_ref=got_n.at[d - 1], send_sem=lead_send, recv_sem=lead_recv,
                device_id={"tp": lax.rem(tp + d, m)}, device_id_type=MESH,
            )

        def lead_to_row(d):
            return pltpu.make_async_remote_copy(
                src_ref=out_n, dst_ref=out_n, send_sem=last_send, recv_sem=last_recv,
                device_id={"rows": lax.rem(me + d, n)}, device_id_type=MESH,
            )

        def gather_rows():
            wait_for(tile_recv, rows_n.at[pl.ds(0, n - 1)])
            rows_n[me] = tile_n[...]
            deep = m * short // 128
            for y in range(n):
                flat_n[y * deep : (y + 1) * deep, :] = rows_n[y, 0:deep, :]
            flat_16[...] = flat_n[...].astype(jnp.bfloat16)
            pl.semaphore_wait(barrier, m - 1)
            for d in range(1, m):
                lead_to_tp(d).start()

        def gather_tp():
            wait_for(lead_recv, got_n)
            wait_for(lead_send, got_n)
            all_n = flat_16[...].astype(jnp.float32)
            for d in range(1, m):
                all_n = all_n + got_n[d - 1].astype(jnp.float32)
            out_n[...] = all_n.astype(jnp.bfloat16)
            for d in range(1, n):
                lead_to_row(d).start()

        for step in range(2, n // 2 + 1):
            for c in live:
                for way in range(2):
                    if step == 2 and c == 0:
                        early_to(way).wait_recv()
                        serve_piece(0, early.at[way], lax.rem(me + ways[1 - way], n))
                    else:
                        wait_for(recv.at[way, step - 2, c], serve.at[pl.ds(*pieces[c]), pl.ds(0, wide)])
                    if piece(way, step, c) is not None:
                        hop(way, step, c).start()
            if step == 2:
                wait_for(sum_send, sums.at[pl.ds(0, n - 1)])
                if first > 0:
                    wait_for(early_send, early.at[:, pl.ds(0, first), :])
                pl.when(leads)(gather_rows)

                @pl.when(jnp.logical_not(leads))
                def _():
                    tile_to_lead().wait_send()

            if step == n // 2 - 1:
                pl.when(leads)(gather_tp)

        for way in range(2):
            wait_for(final_recv.at[way], bufs.at[pl.ds(0, columns // 4), :])
        for way in range(2):
            hops = (n // 2 - 1) * columns + columns // 2 - first
            wait_for(send.at[way], bufs.at[pl.ds(0, hops // 2), :])

        @pl.when(leads)
        def _():
            wait_for(last_send, got_n.at[pl.ds(0, n - 1)])

        @pl.when(jnp.logical_not(leads))
        def _():
            wait_for(last_recv, out_n)

    ring0 = (lax.axis_index("copy") == 0) & (tp < 2)
    core = lax.rem(tp, 2)
    for k, first in enumerate(EARLY):
        pl.when((core == k % 2) & (ring0 == (k >= 2)))(functools.partial(rest, first))


def put_out(
    serve, whole, col_q, col_k, col_v, norm,
    out_q, out_k, out_v, out_col_q, out_col_k, out_col_v, out_n, whole_q, whole_k, whole_v,
    sem,
):
    copies = []

    def put(src, dst):
        copies.append(pltpu.make_async_copy(src, dst, sem.at[len(copies)]))
        copies[-1].start()

    for src, dsts in ((serve, (out_q, out_k, out_v)), (whole, (whole_q, whole_k, whole_v))):
        at = 0
        for dst in dsts:
            put(src.at[pl.ds(at, dst.shape[0]), :], dst)
            at += dst.shape[0]
    for src, dst in ((col_q, out_col_q), (col_k, out_col_k), (col_v, out_col_v)):
        put(src.at[0], dst)
    put(norm, out_n)
    for copy in copies:
        copy.wait()


def local(n, m, *args):
    arrays = [pltpu.with_memory_space_constraint(a.T, pltpu.HBM) for a in args[:9]]
    norm = [pltpu.with_memory_space_constraint(a.reshape(1, -1), pltpu.HBM) for a in args[9:]]
    sizes = [arrays[i].shape[0] for i in (0, 3, 6)]
    columns, wide = sum(sizes), arrays[0].shape[1]
    f32, bf16 = jnp.float32, jnp.bfloat16
    length = n * m * norm[0].shape[1]
    flat = (length // 128, 128)
    count = max(len(pieces_of(columns, first)) for first in EARLY)
    dma, vmem, shape = pltpu.SemaphoreType.DMA, pltpu.VMEM, jax.ShapeDtypeStruct
    held = [
        shape((columns, n * wide), bf16),
        shape((columns, wide), f32),
        *[shape((1, size), f32) for size in sizes],
        shape(flat, bf16),
    ]
    outs = pl.pallas_call(
        functools.partial(kernel, n, m),
        out_shape=held,
        in_specs=[pl.BlockSpec(memory_space=pltpu.HBM)] * 11,
        out_specs=[pl.BlockSpec(memory_space=vmem)] * len(held),
        scratch_shapes=[
            vmem((3 * columns, wide), f32),
            vmem((2, 1, norm[0].shape[1]), f32),
            vmem((n, 8, 128), f32),
            vmem((8, 128), f32),
            vmem((n, 8, 128), f32),
            vmem(flat, f32),
            vmem(flat, bf16),
            vmem((m - 1, *flat), bf16),
            vmem((2, max(EARLY), wide), f32),
            dma((columns // LOAD,)),
            dma,
            dma,
            dma,
            dma((2,)),
            dma((2, n // 2 - 1, count)),
            dma((2,)),
            pltpu.SemaphoreType.REGULAR,
            dma,
            dma((2,)),
            *[dma] * 6,
        ],
        compiler_params=pltpu.CompilerParams(
            collective_id=0, has_side_effects=True, vmem_limit_bytes=32 * 1024 * 1024
        ),
        name="step_and_gather",
    )(*arrays, *norm)
    results = [
        *[shape((size, n * wide), bf16) for size in sizes],
        *[shape((size,), f32) for size in sizes],
        shape(flat, bf16),
        *[shape((size, wide), f32) for size in sizes],
    ]
    outs = pl.pallas_call(
        put_out,
        out_shape=results,
        in_specs=[pl.BlockSpec(memory_space=vmem)] * len(held),
        out_specs=[pl.BlockSpec(memory_space=pltpu.HBM)] * len(results),
        scratch_shapes=[dma((len(results),))],
        compiler_params=pltpu.CompilerParams(vmem_limit_bytes=8 * 1024 * 1024),
        name="put_out",
    )(*outs)
    serving, scales, gain, kept = outs[:3], outs[3:6], outs[6], outs[7:]
    return (*[a.T for a in serving], *scales, gain.reshape(-1), *[a.T for a in kept])


def solution(mesh):
    n, m = mesh.shape["rows"], mesh.shape["tp"]
    trained = P(("copy", "rows"), "tp")
    gains = P(("copy", "rows", "tp"))
    in_specs = (trained,) * 9 + (gains,) * 2
    out_specs = (P("copy", "tp"),) * 3 + (P(("copy", "tp")),) * 3 + (P("copy"),) + (trained,) * 3
    return jax.shard_map(
        functools.partial(local, n, m), mesh=mesh, in_specs=in_specs, out_specs=out_specs, check_vma=False
    )
```

```python
import functools

import jax
import jax.numpy as jnp
from jax import lax
from jax.experimental import pallas as pl
from jax.experimental.pallas import tpu as pltpu
from jax.sharding import PartitionSpec as P

D_MODEL = 5120
MESH = pl.DeviceIdType.MESH

learn_rate = 0.01
decay_rate = 0.1
tiny_value = 1e-08

LOAD = 64
GROUPS = (2, 2, 2, 1)
PIECES = ((64, 128, 128, 128), (48, 144, 128, 128), (0, 128, 128, 128, 64), (96, 96, 128, 128))


def pieces_of(sizes):
    return [(sum(sizes[:c]), size) for c, size in enumerate(sizes)]


def last_part(columns, way, at, size):
    low = max(at, way * columns // 2)
    high = min(at + size, (way + 1) * columns // 2)
    return (low, high - low) if low < high else None


def slots_of(n, columns, sizes):
    slots = []
    for c, (at, size) in enumerate(pieces_of(sizes)):
        for way in range(2):
            for step in range(1, n // 2):
                on = step < n // 2 - 1 or last_part(columns, way, at, size) is not None
                if size > 0 and on and (step, c) != (1, 0):
                    slots.append((way, step, c))
    return slots


def wait_for(sem, ref):
    pltpu.make_async_copy(ref, ref, sem).wait()


def kernel(
    n,
    m,
    tq, dq, sq, tk, dk, sk, tv, dv, sv, nt, ns,
    serve, whole, col_q, col_k, col_v, out_n,
    bufs, norm_in, sums, tile_n, rows_n, flat_n, flat_16, got_n, early,
    in_sem, norm_sem, sum_send, sum_recv, send, recv, final_recv, ready, early_send, early_recv,
    tile_send, tile_recv, lead_send, lead_recv, last_send, last_recv,
):
    me = lax.axis_index("rows")
    tp = lax.axis_index("tp")
    columns, wide = whole.shape
    loads = []
    for refs in ((tq, dq, sq), (tk, dk, sk), (tv, dv, sv)):
        loads += [(refs, at) for at in range(0, refs[0].shape[0], LOAD)]
    ways = (1, n - 1)

    lead = n // 4
    leads = me == lead
    barrier = pltpu.get_barrier_semaphore()
    for d in range(1, n):
        peer = lax.rem(me + d, n)

        @pl.when(peer != lead)
        def _():
            pl.semaphore_signal(barrier, inc=1, device_id={"rows": peer}, device_id_type=MESH)

    def place(c, i):
        return pl.ds((c * 3 + i) * LOAD, LOAD)

    group = [g for g, size in enumerate(GROUPS) for _ in range(size)]
    for c, (refs, at) in enumerate(loads):
        for i in range(3):
            pltpu.make_async_copy(refs[i].at[pl.ds(at, LOAD), :], bufs.at[place(c, i), :], in_sem.at[group[c]]).start()
    for i, ref in enumerate((nt, ns)):
        pltpu.make_async_copy(ref, norm_in.at[i], norm_sem).start()

    @pl.when(leads)
    def _():
        for d in range(1, m):
            pl.semaphore_signal(barrier, inc=1, device_id={"tp": lax.rem(tp + d, m)}, device_id_type=MESH)

    lane = lax.broadcasted_iota(jnp.int32, (8, 128), 1)
    sub = lax.broadcasted_iota(jnp.int32, (8, 128), 0)

    total = jnp.zeros((8, 128), jnp.float32)
    for c in range(len(loads)):
        if c == 0 or group[c] != group[c - 1]:
            wait_for(in_sem.at[group[c]], bufs.at[pl.ds(c * 3 * LOAD, GROUPS[group[c]] * 3 * LOAD), :])
        for r in range(0, LOAD, 8):
            t, d, s = (bufs[(c * 3 + i) * LOAD + r : (c * 3 + i) * LOAD + r + 8, :] for i in range(3))
            w = t - learn_rate * (d / (jnp.sqrt(s) + tiny_value) + decay_rate * t)
            at = c * LOAD + r
            whole[at : at + 8, :] = w
            part = jnp.sum(jnp.abs(w), axis=1, keepdims=True)
            total = jnp.where(lane == at // 8, part, total)
    sums[me] = total

    @pl.when(jnp.logical_not(leads))
    def _():
        pl.semaphore_wait(barrier, n - 1)

    @pl.when(me == lead + 1)
    def _():
        pl.semaphore_signal(ready, inc=1, device_id={"rows": lead}, device_id_type=MESH)

    @pl.when(leads)
    def _():
        pl.semaphore_wait(ready, 1)

    for d in (n // 2, *[x for k in range(n // 2 - 1, 0, -1) for x in (k, n - k)]):
        pltpu.make_async_remote_copy(
            src_ref=sums.at[me], dst_ref=sums.at[me], send_sem=sum_send, recv_sem=sum_recv,
            device_id={"rows": lax.rem(me + d, n)}, device_id_type=MESH,
        ).start()

    short = nt.shape[1]

    def tile_to_lead():
        return pltpu.make_async_remote_copy(
            src_ref=tile_n, dst_ref=rows_n.at[me], send_sem=tile_send, recv_sem=tile_recv,
            device_id={"rows": lead}, device_id_type=MESH,
        )

    def place_gain():
        wait_for(norm_sem, norm_in)
        gain = norm_in[0] + norm_in[1]
        padded = jnp.concatenate([gain, jnp.zeros((1, 128 - short), jnp.float32)], axis=1)
        turned = pltpu.roll(jnp.broadcast_to(padded, (8, 128)), lax.rem(tp * short, 128), 1)
        spot = sub * 128 + lane - tp * short
        tile_n[...] = jnp.where((spot >= 0) & (spot < short), turned, 0.0)

        @pl.when(jnp.logical_not(leads))
        def _():
            tile_to_lead().start()

    def rest(sizes):
        pieces, first = pieces_of(sizes), sizes[0]
        live = [c for c, (at, size) in enumerate(pieces) if size > 0]

        def early_to(way):
            return pltpu.make_async_remote_copy(
                src_ref=whole.at[pl.ds(0, first), :], dst_ref=early.at[way, pl.ds(0, first), :],
                send_sem=early_send, recv_sem=early_recv.at[way],
                device_id={"rows": lax.rem(me + ways[way], n)}, device_id_type=MESH,
            )

        if first > 0:
            for way in range(2):
                early_to(way).start()
        place_gain()

        wait_for(sum_recv, sums.at[pl.ds(0, n - 1)])
        every = sums[0]
        for y in range(1, n):
            every = every + sums[y]
        column = every / D_MODEL
        inverse = 1.0 / column

        slots = slots_of(n, columns, sizes)

        def piece(way, step, c):
            return pieces[c] if step < n // 2 else last_part(columns, way, *pieces[c])

        def arrival(way, step, c):
            key = (way, step, c)
            return recv.at[slots.index(key)] if key in slots else final_recv.at[way]

        def hop(way, step, c):
            at, size = piece(way, step, c)
            owner = lax.rem(me + (step - 1) * ways[1 - way], n)
            block = serve.at[pl.ds(at, size), pl.ds(pl.multiple_of(owner * wide, 128), wide)]
            return pltpu.make_async_remote_copy(
                src_ref=block, dst_ref=block, send_sem=send.at[way],
                recv_sem=arrival(way, step, c),
                device_id={"rows": lax.rem(me + ways[way], n)}, device_id_type=MESH,
            )

        def serve_piece(c, source, owner):
            at, size = pieces[c]
            here = pl.ds(pl.multiple_of(owner * wide, 128), wide)
            for r in range(0, size, 16):
                both = []
                for h in range(r, r + 16, 8):
                    g = (at + h) // 8
                    scale = jnp.broadcast_to(inverse[:, g : g + 1], (8, wide))
                    both.append(source[h : h + 8, :] * scale)
                serve[at + r : at + r + 16, here] = jnp.concatenate(both, axis=0).astype(jnp.bfloat16)

        ahead = live[:1] if first > 0 else []
        orders = [ahead + live[len(ahead) :], ahead + live[len(ahead) :][::-1]]
        done, put = [], [len(ahead)] * 2
        for pair in zip(*(order[len(ahead) :] for order in orders)):
            for c in pair:
                if c not in done:
                    serve_piece(c, whole.at[pl.ds(*pieces[c]), :], me)
                    done.append(c)
            for way, order in enumerate(orders):
                while put[way] < len(order) and order[put[way]] in done:
                    hop(way, 1, order[put[way]]).start()
                    put[way] += 1
        if first > 0:
            serve_piece(0, whole.at[pl.ds(0, first), :], me)

        flat = [jnp.zeros((8, 128), jnp.float32) for _ in range(4)]
        for g in range(columns // 8):
            here = (lane // 8 == g % 16) & (sub == lane % 8)
            flat[g // 16] = jnp.where(here, jnp.broadcast_to(column[:, g : g + 1], (8, 128)), flat[g // 16])
        row = jnp.concatenate([jnp.sum(f, axis=0, keepdims=True) for f in flat], axis=1)
        at = 0
        for ref in (col_q, col_k, col_v):
            size = ref.shape[1]
            ref[...] = row[:, at : at + size]
            at += size

        def lead_to_tp(d):
            return pltpu.make_async_remote_copy(
                src_ref=flat_16, dst_ref=got_n.at[d - 1], send_sem=lead_send, recv_sem=lead_recv,
                device_id={"tp": lax.rem(tp + d, m)}, device_id_type=MESH,
            )

        def lead_to_row(d):
            return pltpu.make_async_remote_copy(
                src_ref=out_n, dst_ref=out_n, send_sem=last_send, recv_sem=last_recv,
                device_id={"rows": lax.rem(me + d, n)}, device_id_type=MESH,
            )

        def gather_rows():
            wait_for(tile_recv, rows_n.at[pl.ds(0, n - 1)])
            rows_n[me] = tile_n[...]
            deep = m * short // 128
            for y in range(n):
                flat_n[y * deep : (y + 1) * deep, :] = rows_n[y, 0:deep, :]
            flat_16[...] = flat_n[...].astype(jnp.bfloat16)
            pl.semaphore_wait(barrier, m - 1)
            for d in range(1, m):
                lead_to_tp(d).start()

        def gather_tp():
            wait_for(lead_recv, got_n)
            wait_for(lead_send, got_n)
            all_n = flat_16[...].astype(jnp.float32)
            for d in range(1, m):
                all_n = all_n + got_n[d - 1].astype(jnp.float32)
            out_n[...] = all_n.astype(jnp.bfloat16)
            for d in range(1, n):
                lead_to_row(d).start()

        for step in range(2, n // 2 + 1):
            for pair in zip(*orders):
                for way, c in enumerate(pair):
                    if step == 2 and c == 0:
                        early_to(way).wait_recv()
                        serve_piece(0, early.at[way], lax.rem(me + ways[1 - way], n))
                    elif (way, step - 1, c) in slots:
                        wait_for(arrival(way, step - 1, c), serve.at[pl.ds(*pieces[c]), pl.ds(0, wide)])
                    if piece(way, step, c) is not None:
                        hop(way, step, c).start()
            if step == 2:
                wait_for(sum_send, sums.at[pl.ds(0, n - 1)])
                if first > 0:
                    wait_for(early_send, early.at[:, pl.ds(0, first), :])
                pl.when(leads)(gather_rows)

                @pl.when(jnp.logical_not(leads))
                def _():
                    tile_to_lead().wait_send()

            if step == n // 2 - 1:
                pl.when(leads)(gather_tp)

        for way in range(2):
            last = columns // 2
            for c in live:
                last += pieces[c][1] if (way, n // 2 - 1, c) not in slots else 0
            wait_for(final_recv.at[way], bufs.at[pl.ds(0, last // 2), :])
        for way in range(2):
            hops = (n // 2 - 1) * columns + columns // 2 - first
            wait_for(send.at[way], bufs.at[pl.ds(0, hops // 2), :])

        @pl.when(leads)
        def _():
            wait_for(last_send, got_n.at[pl.ds(0, n - 1)])

        @pl.when(jnp.logical_not(leads))
        def _():
            wait_for(last_recv, out_n)

    ring0 = (lax.axis_index("copy") == 0) & (tp < 2)
    core = lax.rem(tp, 2)
    for k, sizes in enumerate(PIECES):
        pl.when((core == k % 2) & (ring0 == (k >= 2)))(functools.partial(rest, sizes))


def put_out(
    serve, whole, col_q, col_k, col_v, norm,
    out_q, out_k, out_v, out_col_q, out_col_k, out_col_v, out_n, whole_q, whole_k, whole_v,
    sem,
):
    for k, (src, dsts) in enumerate(((serve, (out_q, out_k, out_v)), (whole, (whole_q, whole_k, whole_v)))):
        at = 0
        for dst in dsts:
            pltpu.make_async_copy(src.at[pl.ds(at, dst.shape[0]), :], dst, sem.at[k]).start()
            at += dst.shape[0]
    small = ((col_q.at[0], out_col_q), (col_k.at[0], out_col_k), (col_v.at[0], out_col_v), (norm, out_n))
    copies = [pltpu.make_async_copy(*pair, sem.at[2 + k]) for k, pair in enumerate(small)]
    for copy in copies:
        copy.start()
    for copy in copies:
        copy.wait()
    for k, src in enumerate((serve, whole)):
        wait_for(sem.at[k], src)


def local(n, m, *args):
    arrays = [pltpu.with_memory_space_constraint(a.T, pltpu.HBM) for a in args[:9]]
    norm = [pltpu.with_memory_space_constraint(a.reshape(1, -1), pltpu.HBM) for a in args[9:]]
    sizes = [arrays[i].shape[0] for i in (0, 3, 6)]
    columns, wide = sum(sizes), arrays[0].shape[1]
    f32, bf16 = jnp.float32, jnp.bfloat16
    length = n * m * norm[0].shape[1]
    flat = (length // 128, 128)
    count = max(len(slots_of(n, columns, pieces)) for pieces in PIECES)
    dma, vmem, shape = pltpu.SemaphoreType.DMA, pltpu.VMEM, jax.ShapeDtypeStruct
    held = [
        shape((columns, n * wide), bf16),
        shape((columns, wide), f32),
        *[shape((1, size), f32) for size in sizes],
        shape(flat, bf16),
    ]
    outs = pl.pallas_call(
        functools.partial(kernel, n, m),
        out_shape=held,
        in_specs=[pl.BlockSpec(memory_space=pltpu.HBM)] * 11,
        out_specs=[pl.BlockSpec(memory_space=vmem)] * len(held),
        scratch_shapes=[
            vmem((3 * columns, wide), f32),
            vmem((2, 1, norm[0].shape[1]), f32),
            vmem((n, 8, 128), f32),
            vmem((8, 128), f32),
            vmem((n, 8, 128), f32),
            vmem(flat, f32),
            vmem(flat, bf16),
            vmem((m - 1, *flat), bf16),
            vmem((2, max(pieces[0] for pieces in PIECES), wide), f32),
            dma((len(GROUPS),)),
            dma,
            dma,
            dma,
            dma((2,)),
            dma((count,)),
            dma((2,)),
            pltpu.SemaphoreType.REGULAR,
            dma,
            dma((2,)),
            *[dma] * 6,
        ],
        compiler_params=pltpu.CompilerParams(
            collective_id=0, has_side_effects=True, vmem_limit_bytes=32 * 1024 * 1024
        ),
        name="step_and_gather",
    )(*arrays, *norm)
    results = [
        *[shape((size, n * wide), bf16) for size in sizes],
        *[shape((size,), f32) for size in sizes],
        shape(flat, bf16),
        *[shape((size, wide), f32) for size in sizes],
    ]
    outs = pl.pallas_call(
        put_out,
        out_shape=results,
        in_specs=[pl.BlockSpec(memory_space=vmem)] * len(held),
        out_specs=[pl.BlockSpec(memory_space=pltpu.HBM)] * len(results),
        scratch_shapes=[dma((6,))],
        compiler_params=pltpu.CompilerParams(vmem_limit_bytes=8 * 1024 * 1024),
        name="put_out",
    )(*outs)
    serving, scales, gain, kept = outs[:3], outs[3:6], outs[6], outs[7:]
    return (*[a.T for a in serving], *scales, gain.reshape(-1), *[a.T for a in kept])


def solution(mesh):
    n, m = mesh.shape["rows"], mesh.shape["tp"]
    trained = P(("copy", "rows"), "tp")
    gains = P(("copy", "rows", "tp"))
    in_specs = (trained,) * 9 + (gains,) * 2
    out_specs = (P("copy", "tp"),) * 3 + (P(("copy", "tp")),) * 3 + (P("copy"),) + (trained,) * 3
    return jax.shard_map(
        functools.partial(local, n, m), mesh=mesh, in_specs=in_specs, out_specs=out_specs, check_vma=False
    )
```

```python
import functools

import jax
import jax.numpy as jnp
from jax import lax
from jax.experimental import pallas as pl
from jax.experimental.pallas import tpu as pltpu
from jax.sharding import PartitionSpec as P

D_MODEL = 5120
MESH = pl.DeviceIdType.MESH

learn_rate = 0.01
decay_rate = 0.1
tiny_value = 1e-08

LOAD = 64
GROUPS = (2, 2, 2, 1)
PIECES = ((64, 128, 128, 128), (48, 144, 128, 128), (0, 128, 128, 128, 64), (96, 96, 128, 128))


def pieces_of(sizes):
    return [(sum(sizes[:c]), size) for c, size in enumerate(sizes)]


def last_part(columns, way, at, size):
    low = max(at, way * columns // 2)
    high = min(at + size, (way + 1) * columns // 2)
    return (low, high - low) if low < high else None


def slots_of(n, columns, sizes):
    slots = []
    for c, (at, size) in enumerate(pieces_of(sizes)):
        for way in range(2):
            for step in range(1, n // 2):
                on = step < n // 2 - 1 or last_part(columns, way, at, size) is not None
                if size > 0 and on and (step, c) != (1, 0):
                    slots.append((way, step, c))
    return slots


def wait_for(sem, ref):
    pltpu.make_async_copy(ref, ref, sem).wait()


def kernel(
    n,
    m,
    tq, dq, sq, tk, dk, sk, tv, dv, sv, nt, ns,
    serve, whole, col_q, col_k, col_v, out_n,
    bufs, norm_in, sums, tile_n, rows_n, flat_n, flat_16, got_n, early,
    in_sem, norm_sem, sum_send, sum_recv, send, recv, final_recv, ready, early_send, early_recv,
    tile_send, tile_recv, lead_send, lead_recv, last_send, last_recv,
):
    me = lax.axis_index("rows")
    tp = lax.axis_index("tp")
    columns, wide = whole.shape
    loads = []
    for refs in ((tq, dq, sq), (tk, dk, sk), (tv, dv, sv)):
        loads += [(refs, at) for at in range(0, refs[0].shape[0], LOAD)]
    ways = (1, n - 1)

    lead = n // 4
    leads = me == lead
    barrier = pltpu.get_barrier_semaphore()
    for d in range(1, n):
        peer = lax.rem(me + d, n)

        @pl.when(peer != lead)
        def _():
            pl.semaphore_signal(barrier, inc=1, device_id={"rows": peer}, device_id_type=MESH)

    group = [g for g, size in enumerate(GROUPS) for _ in range(size)]
    for c, (refs, at) in enumerate(loads):
        for i in range(3):
            for half in range(0, LOAD, LOAD // 2):
                source = refs[i].at[pl.ds(at + half, LOAD // 2), :]
                here = bufs.at[pl.ds((c * 3 + i) * LOAD + half, LOAD // 2), :]
                pltpu.make_async_copy(source, here, in_sem.at[group[c]]).start()
    for i, ref in enumerate((nt, ns)):
        pltpu.make_async_copy(ref, norm_in.at[i], norm_sem).start()

    @pl.when(leads)
    def _():
        for d in range(1, m):
            pl.semaphore_signal(barrier, inc=1, device_id={"tp": lax.rem(tp + d, m)}, device_id_type=MESH)

    lane = lax.broadcasted_iota(jnp.int32, (8, 128), 1)
    sub = lax.broadcasted_iota(jnp.int32, (8, 128), 0)

    total = jnp.zeros((8, 128), jnp.float32)
    for c in range(len(loads)):
        if c == 0 or group[c] != group[c - 1]:
            wait_for(in_sem.at[group[c]], bufs.at[pl.ds(c * 3 * LOAD, GROUPS[group[c]] * 3 * LOAD), :])
        for r in range(0, LOAD, 8):
            t, d, s = (bufs[(c * 3 + i) * LOAD + r : (c * 3 + i) * LOAD + r + 8, :] for i in range(3))
            w = t - learn_rate * (d / (jnp.sqrt(s) + tiny_value) + decay_rate * t)
            at = c * LOAD + r
            whole[at : at + 8, :] = w
            part = jnp.sum(jnp.abs(w), axis=1, keepdims=True)
            total = jnp.where(lane == at // 8, part, total)
    sums[me] = total

    @pl.when(jnp.logical_not(leads))
    def _():
        pl.semaphore_wait(barrier, n - 1)

    @pl.when(me == lead + 1)
    def _():
        pl.semaphore_signal(ready, inc=1, device_id={"rows": lead}, device_id_type=MESH)

    @pl.when(leads)
    def _():
        pl.semaphore_wait(ready, 1)

    for d in (n // 2, *[x for k in range(n // 2 - 1, 0, -1) for x in (k, n - k)]):
        pltpu.make_async_remote_copy(
            src_ref=sums.at[me], dst_ref=sums.at[me], send_sem=sum_send, recv_sem=sum_recv,
            device_id={"rows": lax.rem(me + d, n)}, device_id_type=MESH,
        ).start()

    short = nt.shape[1]

    def tile_to_lead():
        return pltpu.make_async_remote_copy(
            src_ref=tile_n, dst_ref=rows_n.at[me], send_sem=tile_send, recv_sem=tile_recv,
            device_id={"rows": lead}, device_id_type=MESH,
        )

    def place_gain():
        wait_for(norm_sem, norm_in)
        gain = norm_in[0] + norm_in[1]
        padded = jnp.concatenate([gain, jnp.zeros((1, 128 - short), jnp.float32)], axis=1)
        turned = pltpu.roll(jnp.broadcast_to(padded, (8, 128)), lax.rem(tp * short, 128), 1)
        spot = sub * 128 + lane - tp * short
        tile_n[...] = jnp.where((spot >= 0) & (spot < short), turned, 0.0)

        @pl.when(jnp.logical_not(leads))
        def _():
            tile_to_lead().start()

    def rest(sizes):
        pieces, first = pieces_of(sizes), sizes[0]
        live = [c for c, (at, size) in enumerate(pieces) if size > 0]

        def early_to(way):
            return pltpu.make_async_remote_copy(
                src_ref=whole.at[pl.ds(0, first), :], dst_ref=early.at[way, pl.ds(0, first), :],
                send_sem=early_send, recv_sem=early_recv.at[way],
                device_id={"rows": lax.rem(me + ways[way], n)}, device_id_type=MESH,
            )

        if first > 0:
            for way in range(2):
                early_to(way).start()
        place_gain()

        wait_for(sum_recv, sums.at[pl.ds(0, n - 1)])
        every = sums[0]
        for y in range(1, n):
            every = every + sums[y]
        column = every / D_MODEL
        inverse = 1.0 / column

        slots = slots_of(n, columns, sizes)

        def piece(way, step, c):
            return pieces[c] if step < n // 2 else last_part(columns, way, *pieces[c])

        def arrival(way, step, c):
            key = (way, step, c)
            return recv.at[slots.index(key)] if key in slots else final_recv.at[way]

        def hop(way, step, c):
            at, size = piece(way, step, c)
            owner = lax.rem(me + (step - 1) * ways[1 - way], n)
            block = serve.at[pl.ds(at, size), pl.ds(pl.multiple_of(owner * wide, 128), wide)]
            return pltpu.make_async_remote_copy(
                src_ref=block, dst_ref=block, send_sem=send.at[way],
                recv_sem=arrival(way, step, c),
                device_id={"rows": lax.rem(me + ways[way], n)}, device_id_type=MESH,
            )

        def serve_piece(c, source, owner):
            at, size = pieces[c]
            here = pl.ds(pl.multiple_of(owner * wide, 128), wide)
            for r in range(0, size, 16):
                both = []
                for h in range(r, r + 16, 8):
                    g = (at + h) // 8
                    scale = jnp.broadcast_to(inverse[:, g : g + 1], (8, wide))
                    both.append(source[h : h + 8, :] * scale)
                serve[at + r : at + r + 16, here] = jnp.concatenate(both, axis=0).astype(jnp.bfloat16)

        ahead = live[:1] if first > 0 else []
        orders = [ahead + live[len(ahead) :], ahead + live[len(ahead) :][::-1]]
        done, put = [], [len(ahead)] * 2
        for pair in zip(*(order[len(ahead) :] for order in orders)):
            for c in pair:
                if c not in done:
                    serve_piece(c, whole.at[pl.ds(*pieces[c]), :], me)
                    done.append(c)
            for way, order in enumerate(orders):
                while put[way] < len(order) and order[put[way]] in done:
                    hop(way, 1, order[put[way]]).start()
                    put[way] += 1
        if first > 0:
            serve_piece(0, whole.at[pl.ds(0, first), :], me)

        flat = [jnp.zeros((8, 128), jnp.float32) for _ in range(4)]
        for g in range(columns // 8):
            here = (lane // 8 == g % 16) & (sub == lane % 8)
            flat[g // 16] = jnp.where(here, jnp.broadcast_to(column[:, g : g + 1], (8, 128)), flat[g // 16])
        row = jnp.concatenate([jnp.sum(f, axis=0, keepdims=True) for f in flat], axis=1)
        at = 0
        for ref in (col_q, col_k, col_v):
            size = ref.shape[1]
            ref[...] = row[:, at : at + size]
            at += size

        def lead_to_tp(d):
            return pltpu.make_async_remote_copy(
                src_ref=flat_16, dst_ref=got_n.at[d - 1], send_sem=lead_send, recv_sem=lead_recv,
                device_id={"tp": lax.rem(tp + d, m)}, device_id_type=MESH,
            )

        def lead_to_row(d):
            return pltpu.make_async_remote_copy(
                src_ref=out_n, dst_ref=out_n, send_sem=last_send, recv_sem=last_recv,
                device_id={"rows": lax.rem(me + d, n)}, device_id_type=MESH,
            )

        def gather_rows():
            wait_for(tile_recv, rows_n.at[pl.ds(0, n - 1)])
            rows_n[me] = tile_n[...]
            deep = m * short // 128
            for y in range(n):
                flat_n[y * deep : (y + 1) * deep, :] = rows_n[y, 0:deep, :]
            flat_16[...] = flat_n[...].astype(jnp.bfloat16)
            pl.semaphore_wait(barrier, m - 1)
            for d in range(1, m):
                lead_to_tp(d).start()

        def gather_tp():
            wait_for(lead_recv, got_n)
            wait_for(lead_send, got_n)
            all_n = flat_16[...].astype(jnp.float32)
            for d in range(1, m):
                all_n = all_n + got_n[d - 1].astype(jnp.float32)
            out_n[...] = all_n.astype(jnp.bfloat16)
            for d in range(1, n):
                lead_to_row(d).start()

        for step in range(2, n // 2 + 1):
            for pair in zip(*orders):
                for way, c in enumerate(pair):
                    if step == 2 and c == 0:
                        early_to(way).wait_recv()
                        serve_piece(0, early.at[way], lax.rem(me + ways[1 - way], n))
                    elif (way, step - 1, c) in slots:
                        wait_for(arrival(way, step - 1, c), serve.at[pl.ds(*pieces[c]), pl.ds(0, wide)])
                    if piece(way, step, c) is not None:
                        hop(way, step, c).start()
            if step == 2:
                wait_for(sum_send, sums.at[pl.ds(0, n - 1)])
                if first > 0:
                    wait_for(early_send, early.at[:, pl.ds(0, first), :])
                pl.when(leads)(gather_rows)

                @pl.when(jnp.logical_not(leads))
                def _():
                    tile_to_lead().wait_send()

            if step == n // 2 - 1:
                pl.when(leads)(gather_tp)

        for way in range(2):
            last = columns // 2
            for c in live:
                last += pieces[c][1] if (way, n // 2 - 1, c) not in slots else 0
            wait_for(final_recv.at[way], bufs.at[pl.ds(0, last // 2), :])
        for way in range(2):
            hops = (n // 2 - 1) * columns + columns // 2 - first
            wait_for(send.at[way], bufs.at[pl.ds(0, hops // 2), :])

        @pl.when(leads)
        def _():
            wait_for(last_send, got_n.at[pl.ds(0, n - 1)])

        @pl.when(jnp.logical_not(leads))
        def _():
            wait_for(last_recv, out_n)

    ring0 = (lax.axis_index("copy") == 0) & (tp < 2)
    core = lax.rem(tp, 2)
    for k, sizes in enumerate(PIECES):
        pl.when((core == k % 2) & (ring0 == (k >= 2)))(functools.partial(rest, sizes))


def put_out(
    serve, whole, col_q, col_k, col_v, norm,
    out_q, out_k, out_v, out_col_q, out_col_k, out_col_v, out_n, whole_q, whole_k, whole_v,
    sem,
):
    for k, (src, dsts) in enumerate(((serve, (out_q, out_k, out_v)), (whole, (whole_q, whole_k, whole_v)))):
        at = 0
        for dst in dsts:
            size = max(dst.shape[0] // 4, 32)
            for part in range(0, dst.shape[0], size):
                here, there = pl.ds(at + part, size), pl.ds(part, size)
                pltpu.make_async_copy(src.at[here, :], dst.at[there, :], sem.at[k]).start()
            at += dst.shape[0]
    small = ((col_q.at[0], out_col_q), (col_k.at[0], out_col_k), (col_v.at[0], out_col_v), (norm, out_n))
    copies = [pltpu.make_async_copy(*pair, sem.at[2 + k]) for k, pair in enumerate(small)]
    for copy in copies:
        copy.start()
    for copy in copies:
        copy.wait()
    for k, src in enumerate((serve, whole)):
        wait_for(sem.at[k], src)


def local(n, m, *args):
    arrays = [pltpu.with_memory_space_constraint(a.T, pltpu.HBM) for a in args[:9]]
    norm = [pltpu.with_memory_space_constraint(a.reshape(1, -1), pltpu.HBM) for a in args[9:]]
    sizes = [arrays[i].shape[0] for i in (0, 3, 6)]
    columns, wide = sum(sizes), arrays[0].shape[1]
    f32, bf16 = jnp.float32, jnp.bfloat16
    length = n * m * norm[0].shape[1]
    flat = (length // 128, 128)
    count = max(len(slots_of(n, columns, pieces)) for pieces in PIECES)
    dma, vmem, shape = pltpu.SemaphoreType.DMA, pltpu.VMEM, jax.ShapeDtypeStruct
    held = [
        shape((columns, n * wide), bf16),
        shape((columns, wide), f32),
        *[shape((1, size), f32) for size in sizes],
        shape(flat, bf16),
    ]
    outs = pl.pallas_call(
        functools.partial(kernel, n, m),
        out_shape=held,
        in_specs=[pl.BlockSpec(memory_space=pltpu.HBM)] * 11,
        out_specs=[pl.BlockSpec(memory_space=vmem)] * len(held),
        scratch_shapes=[
            vmem((3 * columns, wide), f32),
            vmem((2, 1, norm[0].shape[1]), f32),
            vmem((n, 8, 128), f32),
            vmem((8, 128), f32),
            vmem((n, 8, 128), f32),
            vmem(flat, f32),
            vmem(flat, bf16),
            vmem((m - 1, *flat), bf16),
            vmem((2, max(pieces[0] for pieces in PIECES), wide), f32),
            dma((len(GROUPS),)),
            dma,
            dma,
            dma,
            dma((2,)),
            dma((count,)),
            dma((2,)),
            pltpu.SemaphoreType.REGULAR,
            dma,
            dma((2,)),
            *[dma] * 6,
        ],
        compiler_params=pltpu.CompilerParams(
            collective_id=0, has_side_effects=True, vmem_limit_bytes=32 * 1024 * 1024
        ),
        name="step_and_gather",
    )(*arrays, *norm)
    results = [
        *[shape((size, n * wide), bf16) for size in sizes],
        *[shape((size,), f32) for size in sizes],
        shape(flat, bf16),
        *[shape((size, wide), f32) for size in sizes],
    ]
    outs = pl.pallas_call(
        put_out,
        out_shape=results,
        in_specs=[pl.BlockSpec(memory_space=vmem)] * len(held),
        out_specs=[pl.BlockSpec(memory_space=pltpu.HBM)] * len(results),
        scratch_shapes=[dma((6,))],
        compiler_params=pltpu.CompilerParams(vmem_limit_bytes=8 * 1024 * 1024),
        name="put_out",
    )(*outs)
    serving, scales, gain, kept = outs[:3], outs[3:6], outs[6], outs[7:]
    return (*[a.T for a in serving], *scales, gain.reshape(-1), *[a.T for a in kept])


def solution(mesh):
    n, m = mesh.shape["rows"], mesh.shape["tp"]
    trained = P(("copy", "rows"), "tp")
    gains = P(("copy", "rows", "tp"))
    in_specs = (trained,) * 9 + (gains,) * 2
    out_specs = (P("copy", "tp"),) * 3 + (P(("copy", "tp")),) * 3 + (P("copy"),) + (trained,) * 3
    return jax.shard_map(
        functools.partial(local, n, m), mesh=mesh, in_specs=in_specs, out_specs=out_specs, check_vma=False
    )
```
